32 devices in a mesh: slab: 16 (over z, y, x), sub: 2 (over core).
Axes of the slice: x: 2, y: 2, z: 4, core: 2. Of those that a mesh axis runs over, the one named last changes fastest.
Arguments:
- start: float32 [4, 96, 32, 256], P(None, 'slab', 'sub'), may hold values from -6 to 6
- wind: float32 [3, 96, 32, 256], P(None, 'slab', 'sub'), may hold values from -4 to 4
- reaction: float32 [96, 32, 256], P('slab', 'sub'), may hold values from 0.5 to 4
- mass: float32 [96, 32, 256], P('slab', 'sub'), may hold values from 0.5 to 2
Outputs:
- basis: float32 [4, 4, 96, 32, 256], P(None, None, 'slab', 'sub')
- search: float32 [3, 4, 96, 32, 256], P(None, None, 'slab', 'sub')
- hessenberg: float32 [4, 3], replicated
The draws below stay inside these ranges and needn't reach their ends.
All inputs are finite; a program needn't handle non-finite values.
Results may differ from the reference program's by a relative error of at most 0.0003.
Values sent between devices are 32-bit elements; how exact they have to be, the bound alone decides.
A program may use at most 64 MiB of HBM per device.

```python
import math
import jax
import jax.numpy as jnp

NZ = 256
ITERS = 3
NX = 96
NY = 32


def level_of(key, shape, split, low, top_value):
    loudness, own = 1.0, jax.random.fold_in(key, 6)
    for axis_at, blocks in split:
        draws = jnp.exp(jax.random.uniform(jax.random.fold_in(own, axis_at), (blocks,), jnp.float32, low / len(split), top_value / len(split)))
        loudness = loudness * jnp.repeat(draws, shape[axis_at] // blocks).reshape([-1 if axis == axis_at else 1 for axis in range(len(shape))])
    return loudness


def normal_values(own_key, shape, spread, reach, split=(), held_as=jnp.bfloat16):
    loudness = level_of(own_key, shape, split, -0.22, 0.18) if split else 1.0
    values = jax.random.normal(own_key, shape, jnp.float32) * spread * loudness
    return jnp.minimum(jnp.maximum(values, -reach), reach).astype(held_as)


def setup_inputs(seed: int = 0) -> dict:
    splits = jax.random.split(jax.random.key(seed), 5)
    return {
        "start": normal_values(splits[0], (4, NX, NY, NZ), 1.0, 6.0, ((1, 16), (2, 2)), jnp.float32),
        "wind": normal_values(splits[1], (3, NX, NY, NZ), 1.0, 4.0, ((1, 16), (2, 2)), jnp.float32),
        "reaction": jnp.clip(jnp.exp(math.log(4.0) - 2.0794415 * jax.random.uniform(splits[2], (NX, NY, NZ), jnp.float32) ** level_of(splits[2], (NX, NY, NZ), ((0, 16), (1, 2)), -0.2, 0.2)), 0.5, 4.0),
        "mass": jnp.clip(jnp.exp(math.log(2.0) - 1.3862944 * jax.random.uniform(splits[3], (NX, NY, NZ), jnp.float32) ** level_of(splits[3], (NX, NY, NZ), ((0, 16), (1, 2)), -0.2, 0.2)), 0.5, 2.0),
    }


def grid_pad(field):
    return jnp.pad(field, [(0, 0)] * (field.ndim - 3) + [(1, 1), (1, 1), (0, 0)])

def neighbour_sets(padded):
    center = padded[..., 1:-1, 1:-1, :]
    zero_face = jnp.zeros_like(center[..., :1])
    plus_side = (padded[..., 2:, 1:-1, :], padded[..., 1:-1, 2:, :], jnp.concatenate([center[..., 1:], zero_face], -1))
    minus_side = (padded[..., :-2, 1:-1, :], padded[..., 1:-1, :-2, :], jnp.concatenate([zero_face, center[..., :-1]], -1))
    return (center, plus_side, minus_side)

def six_sum(plus_side, minus_side):
    total = plus_side[0] + minus_side[0]
    total = total + plus_side[1] + minus_side[1]
    return total + plus_side[2] + minus_side[2]

def transport(padded, reaction_k, wind_k):
    center, plus_side, minus_side = neighbour_sets(padded)
    convect = wind_k[0] * (plus_side[0] - minus_side[0])
    convect = convect + wind_k[1] * (plus_side[1] - minus_side[1])
    convect = convect + wind_k[2] * (plus_side[2] - minus_side[2])
    return (6.0 + reaction_k) * center - six_sum(plus_side, minus_side) + 0.5 * convect

def gradient(padded):
    center, plus_side, minus_side = neighbour_sets(padded)
    return jnp.stack([0.5 * (plus_side[dim_index] - minus_side[dim_index]) for dim_index in range(3)])

def divergence(padded):
    center, plus_side, minus_side = neighbour_sets(padded)
    total = 0.5 * (plus_side[0][0] - minus_side[0][0])
    total = total + 0.5 * (plus_side[1][1] - minus_side[1][1])
    return total + 0.5 * (plus_side[2][2] - minus_side[2][2])

def pressure_poisson(padded):
    center, plus_side, minus_side = neighbour_sets(padded)
    return 7.0 * center - six_sum(plus_side, minus_side)

def oseen_apply(padded, reaction_k, wind_k):
    upper = transport(padded[:3], reaction_k, wind_k) + gradient(padded[3])
    center, plus_side, minus_side = neighbour_sets(padded[3])
    lower = -divergence(padded[:3]) - 0.5 * (6.0 * center - six_sum(plus_side, minus_side))
    return jnp.concatenate([upper, lower[None]], 0)

def precondition(vector, wind, reaction, mass):
    pressure = vector[3]
    first_guess = pressure / 7.0
    second_guess = first_guess + (pressure - pressure_poisson(grid_pad(first_guess))) / 7.0
    schur = -transport(grid_pad(second_guess), reaction, wind) / mass
    residue = vector[:3] - gradient(grid_pad(schur))
    diagonal = 6.0 + reaction
    velocity_first = residue / diagonal
    velocity = velocity_first + (residue - transport(grid_pad(velocity_first), reaction, wind)) / diagonal
    return jnp.concatenate([velocity, schur[None]], 0)

def reference(start, wind, reaction, mass):
    scale_start = jnp.sqrt(jnp.sum(start * start))
    vectors = [start / scale_start]
    searches = []
    hess = jnp.zeros((ITERS + 1, ITERS), jnp.float32)
    for column in range(ITERS):
        found = precondition(vectors[column], wind, reaction, mass)
        searches.append(found)
        image = oseen_apply(grid_pad(found), reaction, wind)
        projected = jnp.stack([jnp.sum(vectors[row] * image) for row in range(column + 1)])
        for row in range(column + 1):
            image = image - projected[row] * vectors[row]
        norm_next = jnp.sqrt(jnp.sum(image * image))
        hess = hess.at[:column + 1, column].set(projected)
        hess = hess.at[column + 1, column].set(norm_next)
        vectors.append(image / norm_next)
    return (jnp.stack(vectors), jnp.stack(searches), hess)
```

```python
import functools

import jax
import jax.numpy as jnp
from jax import lax
from jax.experimental import pallas as pl
from jax.experimental.pallas import tpu as pltpu
from jax.sharding import PartitionSpec as P

ITERS = 3
WP, WU, WC = 5, 2, 3
HALO = 8
LANES = 128
MESH = pl.DeviceIdType.MESH


def fold(x):
    rows, cols = x.shape
    total = None
    for r in range(0, rows, 8):
        for c in range(0, cols, LANES):
            piece = x[r : r + 8, c : c + LANES]
            total = piece if total is None else total + piece
    return total


def kernel(
    slabs, subs, cx, cy, nz,
    start, wind, reaction, mass, basis, search, hess,
    xp, xu, vp, vu, raw, co, mk, t1, qq, y0, y1, wl, ob, os_, red,
    send, recv, red_send, red_recv, load, store,
):
    slab, sub = lax.axis_index("slab"), lax.axis_index("sub")
    n = slabs * subs
    me = slab * subs + sub
    rows = cy + HALO
    has_left, has_right = slab > 0, slab < slabs - 1

    loads = [
        pltpu.make_async_copy(start.at[3], xp.at[0, pl.ds(WP, cx), pl.ds(0, cy)], load.at[0]),
        pltpu.make_async_copy(
            start.at[pl.ds(0, 3)], xu.at[0, :, pl.ds(WU, cx), pl.ds(0, cy)], load.at[1]
        ),
        pltpu.make_async_copy(
            wind, raw.at[pl.ds(0, 3), pl.ds(WC, cx), pl.ds(0, cy)], load.at[2]
        ),
        pltpu.make_async_copy(reaction, raw.at[3, pl.ds(WC, cx), pl.ds(0, cy)], load.at[3]),
        pltpu.make_async_copy(mass, raw.at[4, pl.ds(WC, cx), pl.ds(0, cy)], load.at[4]),
    ]
    for item in loads:
        item.start()

    barrier = pltpu.get_barrier_semaphore()

    def greet(k, carry):
        other = lax.rem(me + k, n)
        pl.semaphore_signal(
            barrier, inc=1, device_id=(other // subs, other % subs), device_id_type=MESH
        )
        return carry

    lax.fori_loop(1, n, greet, 0)

    def clear(low):
        def inner():
            for e in range(ITERS):
                for k in range(WP):
                    at = k if low else WP + cx + k
                    xp[e, at, 0:cy] = jnp.zeros((cy, nz), jnp.float32)
                for c in range(3):
                    for k in range(WU):
                        at = k if low else WU + cx + k
                        xu[e, c, at, 0:cy] = jnp.zeros((cy, nz), jnp.float32)
            for c in range(5):
                for k in range(WC):
                    at = k if low else WC + cx + k
                    raw[c, at, 0:cy] = jnp.zeros((cy, nz), jnp.float32)
        return inner

    pl.when(jnp.logical_not(has_left))(clear(True))
    pl.when(jnp.logical_not(has_right))(clear(False))

    row = lax.broadcasted_iota(jnp.int32, (rows, nz), 0)
    col = lax.broadcasted_iota(jnp.int32, (rows, nz), 1)
    last = jnp.where(sub == 0, rows - 1, cy - 1)
    first = jnp.where(sub == 0, 0, cy)
    mk[0] = jnp.where(row == last, 0.0, 1.0)
    mk[1] = jnp.where(row == first, 0.0, 1.0)
    mk[2] = jnp.where(col == nz - 1, 0.0, 1.0)
    mk[3] = jnp.where(col == 0, 0.0, 1.0)

    pl.semaphore_wait(barrier, n - 1)

    def p_view(e):
        return lambda planes, lines: xp.at[e, planes, lines]

    def u_view(e):
        return lambda planes, lines: xu.at[e, :, planes, lines]

    def c_view(planes, lines):
        return raw.at[:, planes, lines]

    groups = [
        (p_view(0), WP), (u_view(0), WU), (c_view, WC),
        (p_view(1), WP), (u_view(1), WU), (p_view(2), WP), (u_view(2), WU),
    ]
    own_lines = pl.ds(0, cy)
    edge_lines = pl.ds(pl.multiple_of((1 - sub) * (cy - HALO), 8), HALO)
    halo_lines = pl.ds(cy, HALO)

    def remote(g, kind):
        view, w = groups[g]
        if kind == 0:
            src, dst = view(pl.ds(cx, w), own_lines), view(pl.ds(0, w), own_lines)
            target = {"slab": slab + 1}
        elif kind == 1:
            src, dst = view(pl.ds(w, w), own_lines), view(pl.ds(w + cx, w), own_lines)
            target = {"slab": slab - 1}
        else:
            planes = (pl.ds(w, cx), pl.ds(0, w), pl.ds(w + cx, w))[kind - 2]
            src, dst = view(planes, edge_lines), view(planes, halo_lines)
            target = {"sub": 1 - sub}
        return pltpu.make_async_remote_copy(
            src_ref=src, dst_ref=dst, send_sem=send.at[g, kind], recv_sem=recv.at[g, kind],
            device_id=target, device_id_type=MESH,
        )

    def begin(g):
        pl.when(has_right)(lambda: remote(g, 0).start())
        pl.when(has_left)(lambda: remote(g, 1).start())
        remote(g, 2).start()

    def forward(g):
        pl.when(has_left)(lambda: remote(g, 0).wait_recv())
        remote(g, 3).start()
        pl.when(has_right)(lambda: remote(g, 1).wait_recv())
        remote(g, 4).start()

    def arrive(g):
        for kind in (2, 3, 4):
            remote(g, kind).wait_recv()

    def finish(g):
        pl.when(has_right)(lambda: remote(g, 0).wait_send())
        pl.when(has_left)(lambda: remote(g, 1).wait_send())
        for kind in (2, 3, 4):
            remote(g, kind).wait_send()

    lane = lax.broadcasted_iota(jnp.int32, (1, LANES), 1)

    def reduce_start(e, parts):
        line = jnp.zeros((1, LANES), jnp.float32)
        for i, part in enumerate(parts):
            line = line + jnp.where(lane == i, jnp.sum(fold(part), keepdims=True), 0.0)
        red[e, me] = line

        def push(k, carry):
            other = lax.rem(me + k, n)
            pltpu.make_async_remote_copy(
                src_ref=red.at[e, me], dst_ref=red.at[e, me],
                send_sem=red_send.at[e], recv_sem=red_recv.at[e],
                device_id=(other // subs, other % subs), device_id_type=MESH,
            ).start()
            return carry

        lax.fori_loop(1, n, push, 0)

    def red_wait(e, sem):
        block = red.at[e, pl.ds(0, n - 1)]
        pltpu.make_async_copy(block, block, sem.at[e]).wait()

    def reduce_end(e, count):
        red_wait(e, red_recv)
        total = jnp.sum(red[e], axis=0)
        return [
            jnp.sum(jnp.where(lane == i, total, 0.0), axis=1, keepdims=True)
            for i in range(count)
        ]

    def turn(f):
        return (
            pltpu.roll(f, rows - 1, 0), pltpu.roll(f, 1, 0),
            pltpu.roll(f, nz - 1, 1), pltpu.roll(f, 1, 1),
        )

    def masked(f):
        yp, ym, zp, zm = turn(f)
        return yp * mk[0], ym * mk[1], zp * mk[2], zm * mk[3]

    def off_diagonal(below, around, above, k):
        yp, ym, zp, zm = around
        total = co[0, k] * above + co[1, k] * below
        total = total + (co[2, k] * yp + co[3, k] * ym)
        return total + (co[4, k] * zp + co[5, k] * zm)

    def loop(count, body, init=0):
        return lax.fori_loop(0, count, body, init)

    def inside(k, w):
        at = slab * cx + k - w
        return jnp.logical_and(at >= 0, at < slabs * cx)

    def coefficients():
        def body(k, carry):
            ok = jnp.where(inside(k, WC), 1.0, 0.0)
            keep = jnp.full((rows, nz), ok) > 0.5
            hx, hy, hz = 0.5 * raw[0, k], 0.5 * raw[1, k], 0.5 * raw[2, k]
            co[0, k] = 1.0 - hx
            co[1, k] = 1.0 + hx
            co[2, k] = (1.0 - hy) * mk[0]
            co[3, k] = (1.0 + hy) * mk[1]
            co[4, k] = (1.0 - hz) * mk[2]
            co[5, k] = (1.0 + hz) * mk[3]
            diagonal = 6.0 + raw[3, k]
            co[6, k] = diagonal
            co[7, k] = jnp.where(keep, 1.0 / diagonal, 0.0)
            co[8, k] = jnp.where(keep, 1.0 / raw[4, k], 0.0)
            return carry

        loop(cx + 2 * WC, body)

    def first_guess(p):
        def body(k, carry):
            here = p[k + 1]
            yp, ym, zp, zm = masked(here)
            total = (p[k] + p[k + 2]) + (yp + ym) + (zp + zm)
            ok = jnp.where(inside(k, WP - 1), 1.0 / 7.0, 0.0)
            t1[k] = (here + total * (1.0 / 7.0)) * ok
            return carry

        loop(cx + 2 * (WP - 1), body)

    def schur():
        def body(k, carry):
            here = t1[k + 1]
            off = off_diagonal(t1[k], turn(here), t1[k + 2], k)
            qq[k] = (off - co[6, k] * here) * co[8, k]
            return carry

        loop(cx + 2 * WC, body)

    def velocity_first(u):
        def body(k, carry):
            yp, ym, zp, zm = masked(qq[k + 1])
            scale = co[7, k + 1]
            y0[0, k] = (u[0, k] - 0.5 * (qq[k + 2] - qq[k])) * scale
            y0[1, k] = (u[1, k] - 0.5 * (yp - ym)) * scale
            y0[2, k] = (u[2, k] - 0.5 * (zp - zm)) * scale
            return carry

        loop(cx + 2 * WU, body)

    def velocity_second():
        def body(k, carry):
            scale = co[7, k + 2]
            for c in range(3):
                here = y0[c, k + 1]
                off = off_diagonal(y0[c, k], turn(here), y0[c, k + 2], k + 2)
                y1[c, k] = here + off * scale
            return carry

        loop(cx + 2, body)

    def image(e, vectors):
        def body(k, acc):
            q = qq[k + WC]
            qa, qb = qq[k + WC + 1], qq[k + WC - 1]
            yp, ym, zp, zm = masked(q)
            grads = (0.5 * (qa - qb), 0.5 * (yp - ym), 0.5 * (zp - zm))
            low = 0.5 * ((qa + qb) + (yp + ym) + (zp + zm)) - 3.0 * q
            out = []
            for c in range(3):
                here = y1[c, k + 1]
                below, above = y1[c, k], y1[c, k + 2]
                around = turn(here)
                off = off_diagonal(below, around, above, k + WC)
                w = (co[6, k + WC] * here - off + grads[c])[:cy]
                if c == 0:
                    low = low - 0.5 * (above - below)
                elif c == 1:
                    low = low - 0.5 * (around[0] * mk[0] - around[1] * mk[1])
                else:
                    low = low - 0.5 * (around[2] * mk[2] - around[3] * mk[3])
                os_[e, c, k] = here[:cy]
                out.append(w)
            os_[e, 3, k] = q[:cy]
            out.append(low[:cy])
            if e + 1 < ITERS:
                for c in range(3):
                    xu[e + 1, c, k + WU, 0:cy] = out[c]
                xp[e + 1, k + WP, 0:cy] = out[3]
            else:
                for c in range(4):
                    wl[c, k] = out[c]
            acc = list(acc)
            for i, (p, u) in enumerate(vectors):
                held = [u[c, k + WU, 0:cy] for c in range(3)] + [p[k + WP, 0:cy]]
                term = held[0] * out[0] + held[1] * out[1]
                acc[i + 1] = acc[i + 1] + (term + (held[2] * out[2] + held[3] * out[3]))
                if i == e:
                    term = held[0] * held[0] + held[1] * held[1]
                    acc[0] = acc[0] + (term + (held[2] * held[2] + held[3] * held[3]))
            return tuple(acc)

        zero = jnp.zeros((cy, nz), jnp.float32)
        return loop(cx, body, (zero,) * (e + 2))

    def write_out(e):
        return (
            pltpu.make_async_copy(ob.at[e], basis.at[e], store.at[0, e]),
            pltpu.make_async_copy(os_.at[e], search.at[e], store.at[1, e]),
        )

    def results(e, vector, inverse):
        p, u = vector

        def body(k, carry):
            for c in range(3):
                ob[e, c, k] = u[c, k + WU, 0:cy] * inverse
            ob[e, 3, k] = p[k + WP, 0:cy] * inverse
            for c in range(4):
                os_[e, c, k] = os_[e, c, k] * inverse
            return carry

        loop(cx, body)
        for item in write_out(e):
            item.start()

    loads[0].wait()
    begin(0)
    for item in loads[2:]:
        item.wait()
    begin(2)
    loads[1].wait()
    begin(1)
    forward(0)
    arrive(0)

    vectors = [(xp.at[0], xu.at[0])]
    inverses = []
    entries = {}
    first_guess(vectors[0][0])
    forward(2)
    arrive(2)
    coefficients()
    for e in range(ITERS):
        p, u = vectors[e]
        p_group, u_group = ((0, 1), (3, 4), (5, 6))[e]
        if e > 0:
            first_guess(p)
        schur()
        if e == 0:
            forward(u_group)
            arrive(u_group)
        else:
            forward(u_group)
            arrive(u_group)

            def form_u(k, carry, e=e):
                for c in range(3):
                    total = xu[e, c, k] * factor
                    for g, (_, other) in zip(weights, vectors[:e]):
                        total = total - g * other[c, k]
                    u[c, k] = total
                return carry

            loop(cx + 2 * WU, form_u)
        velocity_first(u)
        velocity_second()
        acc = image(e, vectors)
        reduce_start(e, acc)
        if e + 1 < ITERS:
            begin(p_group + 3 if e == 0 else 5)
            begin(u_group + 3 if e == 0 else 6)
        sums = reduce_end(e, e + 2)
        norm = jnp.sqrt(sums[0])
        factor = 1.0 / norm
        if e > 0:
            entries[(e, e - 1)] = norm
        inverses.append(factor)
        weights = []
        for i in range(e + 1):
            h = sums[i + 1] * inverses[i] * factor
            entries[(i, e)] = h
            weights.append(h * inverses[i])
        results(e, vectors[e], factor)
        if e + 1 < ITERS:
            g_p = (3, 5)[e]
            forward(g_p)
            arrive(g_p)
            new = (vp.at[e], vu.at[e])

            def form_p(k, carry, e=e):
                total = xp[e + 1, k] * factor
                for g, (other, _) in zip(weights, vectors[: e + 1]):
                    total = total - g * other[k]
                vp[e, k] = total
                return carry

            loop(cx + 2 * WP, form_p)
            vectors.append(new)

    def close(k, acc):
        for c in range(4):
            total = wl[c, k] * factor
            for g, (p, u) in zip(weights, vectors):
                held = p[k + WP, 0:cy] if c == 3 else u[c, k + WU, 0:cy]
                total = total - g * held
            ob[ITERS, c, k] = total
            acc = acc + total * total
        return acc

    acc = loop(cx, close, jnp.zeros((cy, nz), jnp.float32))
    reduce_start(ITERS, [acc])
    for g in range(len(groups)):
        finish(g)
    norm = jnp.sqrt(reduce_end(ITERS, 1)[0])
    entries[(ITERS, ITERS - 1)] = norm
    factor = 1.0 / norm

    def scale(k, carry):
        for c in range(4):
            ob[ITERS, c, k] = ob[ITERS, c, k] * factor
        return carry

    loop(cx, scale)
    final = pltpu.make_async_copy(ob.at[ITERS], basis.at[ITERS], store.at[0, ITERS])
    final.start()
    r = lax.broadcasted_iota(jnp.int32, (ITERS + 1, ITERS), 0)
    c = lax.broadcasted_iota(jnp.int32, (ITERS + 1, ITERS), 1)
    table = jnp.zeros((ITERS + 1, ITERS), jnp.float32)
    for (i, j), value in entries.items():
        table = table + jnp.where(jnp.logical_and(r == i, c == j), value, 0.0)
    hess[...] = table
    for e in range(ITERS + 1):
        red_wait(e, red_send)
    for e in range(ITERS):
        for item in write_out(e):
            item.wait()
    final.wait()


def per_device(slabs, subs, start, wind, reaction, mass):
    _, cx, cy, nz = start.shape
    n = slabs * subs
    rows = cy + HALO
    f32 = jnp.float32

    def field(*lead):
        return pltpu.VMEM((*lead, rows, nz), f32)

    out_shape = (
        jax.ShapeDtypeStruct((ITERS + 1, 4, cx, cy, nz), f32),
        jax.ShapeDtypeStruct((ITERS, 4, cx, cy, nz), f32),
        jax.ShapeDtypeStruct((ITERS + 1, ITERS), f32),
    )
    anywhere = pl.BlockSpec(memory_space=pl.ANY)
    return pl.pallas_call(
        functools.partial(kernel, slabs, subs, cx, cy, nz),
        out_shape=out_shape,
        in_specs=[anywhere] * 4,
        out_specs=(anywhere, anywhere, pl.BlockSpec(memory_space=pltpu.VMEM)),
        scratch_shapes=[
            field(ITERS, cx + 2 * WP),
            field(ITERS, 3, cx + 2 * WU),
            field(ITERS - 1, cx + 2 * WP),
            field(ITERS - 1, 3, cx + 2 * WU),
            field(5, cx + 2 * WC),
            field(9, cx + 2 * WC),
            field(4),
            field(cx + 2 * (WP - 1)),
            field(cx + 2 * WC),
            field(3, cx + 2 * WU),
            field(3, cx + 2),
            pltpu.VMEM((4, cx, cy, nz), f32),
            pltpu.VMEM((ITERS + 1, 4, cx, cy, nz), f32),
            pltpu.VMEM((ITERS, 4, cx, cy, nz), f32),
            pltpu.VMEM((ITERS + 1, n, 1, LANES), f32),
            pltpu.SemaphoreType.DMA((7, 5)),
            pltpu.SemaphoreType.DMA((7, 5)),
            pltpu.SemaphoreType.DMA((ITERS + 1,)),
            pltpu.SemaphoreType.DMA((ITERS + 1,)),
            pltpu.SemaphoreType.DMA((5,)),
            pltpu.SemaphoreType.DMA((2, ITERS + 1)),
        ],
        compiler_params=pltpu.CompilerParams(
            collective_id=0, has_side_effects=True, vmem_limit_bytes=40 * 1024 * 1024
        ),
    )(start, wind, reaction, mass)


def solution(mesh):
    slabs, subs = mesh.shape["slab"], mesh.shape["sub"]
    return jax.shard_map(
        functools.partial(per_device, slabs, subs),
        mesh=mesh,
        in_specs=(
            P(None, "slab", "sub", None),
            P(None, "slab", "sub", None),
            P("slab", "sub", None),
            P("slab", "sub", None),
        ),
        out_specs=(P(None, None, "slab", "sub", None), P(None, None, "slab", "sub", None), P()),
        check_vma=False,
    )
```

```python
import functools

import jax
import jax.numpy as jnp
from jax import lax
from jax.experimental import pallas as pl
from jax.experimental.pallas import tpu as pltpu
from jax.sharding import PartitionSpec as P

ITERS = 3
WP, WU, WC, WQ = 2, 2, 2, 3
HALO = 8
LANES = 128
MESH = pl.DeviceIdType.MESH


def fold(x):
    rows, cols = x.shape
    total = None
    for r in range(0, rows, 8):
        for c in range(0, cols, LANES):
            piece = x[r : r + 8, c : c + LANES]
            total = piece if total is None else total + piece
    return total


def kernel(
    slabs, subs, cx, cy, nz,
    start, wind, reaction, mass, basis, search, hess,
    xp, xu, vp, vu, raw, co, mk, t1, qs, y0, y1, wl, ob, os_, red,
    send, recv, red_send, red_recv, load, store,
):
    slab, sub = lax.axis_index("slab"), lax.axis_index("sub")
    n = slabs * subs
    me = slab * subs + sub
    rows = cy + HALO
    has_left, has_right = slab > 0, slab < slabs - 1

    loads = [
        pltpu.make_async_copy(start.at[3], xp.at[0, pl.ds(WP, cx), pl.ds(0, cy)], load.at[0]),
        pltpu.make_async_copy(
            start.at[pl.ds(0, 3)], xu.at[0, :, pl.ds(WU, cx), pl.ds(0, cy)], load.at[1]
        ),
        pltpu.make_async_copy(
            wind, raw.at[pl.ds(0, 3), pl.ds(WC, cx), pl.ds(0, cy)], load.at[2]
        ),
        pltpu.make_async_copy(reaction, raw.at[3, pl.ds(WC, cx), pl.ds(0, cy)], load.at[3]),
        pltpu.make_async_copy(mass, raw.at[4, pl.ds(WC, cx), pl.ds(0, cy)], load.at[4]),
    ]
    for item in loads:
        item.start()

    barrier = pltpu.get_barrier_semaphore()

    def greet(k, carry):
        for other in range(subs):
            pl.semaphore_signal(
                barrier, inc=1, device_id=(lax.rem(slab + k, slabs), other), device_id_type=MESH
            )
        return carry

    for k in range(1, subs):
        pl.semaphore_signal(
            barrier, inc=1, device_id=(slab, lax.rem(sub + k, subs)), device_id_type=MESH
        )
    lax.fori_loop(1, slabs, greet, 0)

    def clear(low):
        def inner():
            for e in range(ITERS):
                for k in range(WP):
                    at = k if low else WP + cx + k
                    xp[e, at, 0:cy] = jnp.zeros((cy, nz), jnp.float32)
                for k in range(WQ):
                    at = k if low else WQ + cx + k
                    qs[e, at, 0:cy] = jnp.zeros((cy, nz), jnp.float32)
                for c in range(3):
                    for k in range(WU):
                        at = k if low else WU + cx + k
                        xu[e, c, at, 0:cy] = jnp.zeros((cy, nz), jnp.float32)
            for c in range(5):
                for k in range(WC):
                    at = k if low else WC + cx + k
                    raw[c, at, 0:cy] = jnp.zeros((cy, nz), jnp.float32)
        return inner

    pl.when(jnp.logical_not(has_left))(clear(True))
    pl.when(jnp.logical_not(has_right))(clear(False))

    row = lax.broadcasted_iota(jnp.int32, (rows, nz), 0)
    col = lax.broadcasted_iota(jnp.int32, (rows, nz), 1)
    last = jnp.where(sub == 0, rows - 1, cy - 1)
    first = jnp.where(sub == 0, 0, cy)
    mk[0] = jnp.where(row == last, 0.0, 1.0)
    mk[1] = jnp.where(row == first, 0.0, 1.0)
    mk[2] = jnp.where(col == nz - 1, 0.0, 1.0)
    mk[3] = jnp.where(col == 0, 0.0, 1.0)

    pl.semaphore_wait(barrier, n - 1)

    def p_view(e):
        return lambda planes, lines: xp.at[e, planes, lines]

    def u_view(e):
        return lambda planes, lines: xu.at[e, :, planes, lines]

    def q_view(e):
        return lambda planes, lines: qs.at[e, planes, lines]

    def wind_view(planes, lines):
        return raw.at[pl.ds(0, 3), planes, lines]

    def row_view(i):
        return lambda planes, lines: raw.at[i, planes, lines]

    every, across = (0, 1, 2, 3, 4), (0, 1, 3, 4)
    groups = [
        (p_view(0), WP, WP, every), (u_view(0), WU, WU, every),
        (row_view(3), WC, WC, every),
        (p_view(1), WP, WP, every), (u_view(1), WU, WU, every),
        (p_view(2), WP, WP, every), (u_view(2), WU, WU, every),
        (wind_view, WC, 1, every), (row_view(4), WC, 0, (2,)),
        (q_view(0), WQ, WQ, across), (q_view(1), WQ, WQ, across), (q_view(2), WQ, WQ, across),
    ]
    own_lines = pl.ds(0, cy)
    edge_lines = pl.ds(pl.multiple_of((1 - sub) * (cy - HALO), 8), HALO)
    halo_lines = pl.ds(cy, HALO)

    def remote(g, kind):
        view, base, w, _ = groups[g]
        end = base + cx
        if kind == 0:
            src, dst = view(pl.ds(end - w, w), own_lines), view(pl.ds(base - w, w), own_lines)
            target = {"slab": slab + 1}
        elif kind == 1:
            src, dst = view(pl.ds(base, w), own_lines), view(pl.ds(end, w), own_lines)
            target = {"slab": slab - 1}
        else:
            planes = (pl.ds(base, cx), pl.ds(base - w, w), pl.ds(end, w))[kind - 2]
            src, dst = view(planes, edge_lines), view(planes, halo_lines)
            target = {"sub": 1 - sub}
        return pltpu.make_async_remote_copy(
            src_ref=src, dst_ref=dst, send_sem=send.at[g, kind], recv_sem=recv.at[g, kind],
            device_id=target, device_id_type=MESH,
        )

    def begin(g):
        kinds = groups[g][3]
        if 0 in kinds:
            pl.when(has_right)(lambda: remote(g, 0).start())
            pl.when(has_left)(lambda: remote(g, 1).start())
        if 2 in kinds:
            remote(g, 2).start()

    def forward(g):
        if 0 in groups[g][3]:
            pl.when(has_left)(lambda: remote(g, 0).wait_recv())
            remote(g, 3).start()
            pl.when(has_right)(lambda: remote(g, 1).wait_recv())
            remote(g, 4).start()

    def arrive(g):
        for kind in groups[g][3]:
            if kind >= 2:
                remote(g, kind).wait_recv()

    def finish(g):
        for kind in groups[g][3]:
            if kind == 0:
                pl.when(has_right)(lambda: remote(g, 0).wait_send())
            elif kind == 1:
                pl.when(has_left)(lambda: remote(g, 1).wait_send())
            else:
                remote(g, kind).wait_send()

    lane = lax.broadcasted_iota(jnp.int32, (1, LANES), 1)

    def reduce_start(e, parts):
        line = jnp.zeros((1, LANES), jnp.float32)
        for i, part in enumerate(parts):
            line = line + jnp.where(lane == i, jnp.sum(fold(part), keepdims=True), 0.0)
        red[e, me] = line

        def tell(at, core):
            pltpu.make_async_remote_copy(
                src_ref=red.at[e, me], dst_ref=red.at[e, me],
                send_sem=red_send.at[e], recv_sem=red_recv.at[e],
                device_id=(at, core), device_id_type=MESH,
            ).start()

        def push(k, carry):
            at = lax.rem(slab + k, slabs)
            for core in range(subs):
                tell(at, core)
            return carry

        lax.fori_loop(1, slabs, push, 0)
        for k in range(1, subs):
            tell(slab, lax.rem(sub + k, subs))

    def red_wait(e, sem):
        block = red.at[e, pl.ds(0, n - 1)]
        pltpu.make_async_copy(block, block, sem.at[e]).wait()

    def reduce_end(e, count):
        red_wait(e, red_recv)
        total = jnp.sum(red[e], axis=0)
        return [
            jnp.sum(jnp.where(lane == i, total, 0.0), axis=1, keepdims=True)
            for i in range(count)
        ]

    def turn(f):
        return (
            pltpu.roll(f, rows - 1, 0), pltpu.roll(f, 1, 0),
            pltpu.roll(f, nz - 1, 1), pltpu.roll(f, 1, 1),
        )

    def masked(f):
        yp, ym, zp, zm = turn(f)
        return yp * mk[0], ym * mk[1], zp * mk[2], zm * mk[3]

    def off_diagonal(below, around, above, k):
        yp, ym, zp, zm = around
        total = co[0, k] * above + co[1, k] * below
        total = total + (co[2, k] * yp + co[3, k] * ym)
        return total + (co[4, k] * zp + co[5, k] * zm)

    def loop(count, body, init=0):
        return lax.fori_loop(0, count, body, init)

    def inside(k, w):
        at = slab * cx + k - w
        return jnp.logical_and(at >= 0, at < slabs * cx)

    def coefficients():
        def body(k, carry):
            ok = jnp.where(inside(k, WC), 1.0, 0.0)
            keep = jnp.full((rows, nz), ok) > 0.5
            hx, hy, hz = 0.5 * raw[0, k], 0.5 * raw[1, k], 0.5 * raw[2, k]
            co[0, k] = 1.0 - hx
            co[1, k] = 1.0 + hx
            co[2, k] = (1.0 - hy) * mk[0]
            co[3, k] = (1.0 + hy) * mk[1]
            co[4, k] = (1.0 - hz) * mk[2]
            co[5, k] = (1.0 + hz) * mk[3]
            diagonal = 6.0 + raw[3, k]
            co[6, k] = diagonal
            co[7, k] = jnp.where(keep, 1.0 / diagonal, 0.0)
            co[8, k] = jnp.where(keep, 1.0 / raw[4, k], 0.0)
            return carry

        loop(cx + 2 * WC, body)

    def first_guess(p):
        def body(k, carry):
            here = p[k + 1]
            yp, ym, zp, zm = masked(here)
            total = (p[k] + p[k + 2]) + (yp + ym) + (zp + zm)
            ok = jnp.where(inside(k, WP - 1), 1.0 / 7.0, 0.0)
            t1[k] = (here + total * (1.0 / 7.0)) * ok
            return carry

        loop(cx + 2 * (WP - 1), body)

    def schur(qq):
        def body(k, carry):
            here = t1[k + 1]
            off = off_diagonal(t1[k], turn(here), t1[k + 2], k + WC)
            qq[k + WQ] = (off - co[6, k + WC] * here) * co[8, k + WC]
            return carry

        loop(cx, body)

    def velocity_first(qq, u):
        def body(k, carry):
            yp, ym, zp, zm = masked(qq[k + 1])
            scale = co[7, k]
            y0[0, k] = (u[0, k] - 0.5 * (qq[k + 2] - qq[k])) * scale
            y0[1, k] = (u[1, k] - 0.5 * (yp - ym)) * scale
            y0[2, k] = (u[2, k] - 0.5 * (zp - zm)) * scale
            return carry

        loop(cx + 2 * WU, body)

    def velocity_second():
        def body(k, carry):
            scale = co[7, k + 1]
            for c in range(3):
                here = y0[c, k + 1]
                off = off_diagonal(y0[c, k], turn(here), y0[c, k + 2], k + 1)
                y1[c, k] = here + off * scale
            return carry

        loop(cx + 2, body)

    def image(e, qq, vectors):
        def body(k, acc):
            q = qq[k + WQ]
            qa, qb = qq[k + WQ + 1], qq[k + WQ - 1]
            yp, ym, zp, zm = masked(q)
            grads = (0.5 * (qa - qb), 0.5 * (yp - ym), 0.5 * (zp - zm))
            low = 0.5 * ((qa + qb) + (yp + ym) + (zp + zm)) - 3.0 * q
            out = []
            for c in range(3):
                here = y1[c, k + 1]
                below, above = y1[c, k], y1[c, k + 2]
                around = turn(here)
                off = off_diagonal(below, around, above, k + WC)
                w = (co[6, k + WC] * here - off + grads[c])[:cy]
                if c == 0:
                    low = low - 0.5 * (above - below)
                elif c == 1:
                    low = low - 0.5 * (around[0] * mk[0] - around[1] * mk[1])
                else:
                    low = low - 0.5 * (around[2] * mk[2] - around[3] * mk[3])
                os_[e, c, k] = here[:cy]
                out.append(w)
            os_[e, 3, k] = q[:cy]
            out.append(low[:cy])
            if e + 1 < ITERS:
                for c in range(3):
                    xu[e + 1, c, k + WU, 0:cy] = out[c]
                xp[e + 1, k + WP, 0:cy] = out[3]
            else:
                for c in range(4):
                    wl[c, k] = out[c]
            acc = list(acc)
            for i, (p, u) in enumerate(vectors):
                held = [u[c, k + WU, 0:cy] for c in range(3)] + [p[k + WP, 0:cy]]
                term = held[0] * out[0] + held[1] * out[1]
                acc[i + 1] = acc[i + 1] + (term + (held[2] * out[2] + held[3] * out[3]))
                if i == e:
                    term = held[0] * held[0] + held[1] * held[1]
                    acc[0] = acc[0] + (term + (held[2] * held[2] + held[3] * held[3]))
            return tuple(acc)

        zero = jnp.zeros((cy, nz), jnp.float32)
        return loop(cx, body, (zero,) * (e + 2))

    def write_out(e):
        return (
            pltpu.make_async_copy(ob.at[e], basis.at[e], store.at[0, e]),
            pltpu.make_async_copy(os_.at[e], search.at[e], store.at[1, e]),
        )

    def results(e, vector, inverse):
        p, u = vector

        def body(k, carry):
            for c in range(3):
                ob[e, c, k] = u[c, k + WU, 0:cy] * inverse
            ob[e, 3, k] = p[k + WP, 0:cy] * inverse
            for c in range(4):
                os_[e, c, k] = os_[e, c, k] * inverse
            return carry

        loop(cx, body)
        for item in write_out(e):
            item.start()

    loads[0].wait()
    begin(0)
    for item in loads[2:]:
        item.wait()
    for g in (2, 7, 8):
        begin(g)
    loads[1].wait()
    begin(1)
    forward(0)
    arrive(0)

    vectors = [(xp.at[0], xu.at[0])]
    inverses = []
    entries = {}
    first_guess(vectors[0][0])
    for g in (2, 7):
        forward(g)
    for g in (2, 7, 8):
        arrive(g)
    coefficients()
    for e in range(ITERS):
        p, u = vectors[e]
        p_group, u_group = ((0, 1), (3, 4), (5, 6))[e]
        if e > 0:
            first_guess(p)
        qq = qs.at[e]
        schur(qq)
        begin(9 + e)
        if e > 0:
            results(e - 1, vectors[e - 1], inverses[e - 1])
        forward(u_group)
        arrive(u_group)
        if e > 0:

            def form_u(k, carry, e=e):
                for c in range(3):
                    total = xu[e, c, k] * factor
                    for g, (_, other) in zip(weights, vectors[:e]):
                        total = total - g * other[c, k]
                    u[c, k] = total
                return carry

            loop(cx + 2 * WU, form_u)
        forward(9 + e)
        arrive(9 + e)
        velocity_first(qq, u)
        velocity_second()
        acc = image(e, qq, vectors)
        reduce_start(e, acc)
        if e + 1 < ITERS:
            begin(p_group + 3 if e == 0 else 5)
            begin(u_group + 3 if e == 0 else 6)
        sums = reduce_end(e, e + 2)
        norm = jnp.sqrt(sums[0])
        factor = 1.0 / norm
        if e > 0:
            entries[(e, e - 1)] = norm
        inverses.append(factor)
        weights = []
        for i in range(e + 1):
            h = sums[i + 1] * inverses[i] * factor
            entries[(i, e)] = h
            weights.append(h * inverses[i])
        if e + 1 < ITERS:
            g_p = (3, 5)[e]
            forward(g_p)
            arrive(g_p)
            new = (vp.at[e], vu.at[e])

            def form_p(k, carry, e=e):
                total = xp[e + 1, k] * factor
                for g, (other, _) in zip(weights, vectors[: e + 1]):
                    total = total - g * other[k]
                vp[e, k] = total
                return carry

            loop(cx + 2 * WP, form_p)
            vectors.append(new)

    def close(k, acc):
        for c in range(4):
            total = wl[c, k] * factor
            for g, (p, u) in zip(weights, vectors):
                held = p[k + WP, 0:cy] if c == 3 else u[c, k + WU, 0:cy]
                total = total - g * held
            ob[ITERS, c, k] = total
            acc = acc + total * total
        return acc

    acc = loop(cx, close, jnp.zeros((cy, nz), jnp.float32))
    reduce_start(ITERS, [acc])
    results(ITERS - 1, vectors[ITERS - 1], inverses[ITERS - 1])
    for g in range(len(groups)):
        finish(g)
    norm = jnp.sqrt(reduce_end(ITERS, 1)[0])
    entries[(ITERS, ITERS - 1)] = norm
    factor = 1.0 / norm

    def scale(k, carry):
        for c in range(4):
            ob[ITERS, c, k] = ob[ITERS, c, k] * factor
        return carry

    loop(cx, scale)
    final = pltpu.make_async_copy(ob.at[ITERS], basis.at[ITERS], store.at[0, ITERS])
    final.start()
    r = lax.broadcasted_iota(jnp.int32, (ITERS + 1, ITERS), 0)
    c = lax.broadcasted_iota(jnp.int32, (ITERS + 1, ITERS), 1)
    table = jnp.zeros((ITERS + 1, ITERS), jnp.float32)
    for (i, j), value in entries.items():
        table = table + jnp.where(jnp.logical_and(r == i, c == j), value, 0.0)
    hess[...] = table
    for e in range(ITERS + 1):
        red_wait(e, red_send)
    for e in range(ITERS):
        for item in write_out(e):
            item.wait()
    final.wait()


def per_device(slabs, subs, start, wind, reaction, mass):
    _, cx, cy, nz = start.shape
    n = slabs * subs
    rows = cy + HALO
    f32 = jnp.float32

    def field(*lead):
        return pltpu.VMEM((*lead, rows, nz), f32)

    out_shape = (
        jax.ShapeDtypeStruct((ITERS + 1, 4, cx, cy, nz), f32),
        jax.ShapeDtypeStruct((ITERS, 4, cx, cy, nz), f32),
        jax.ShapeDtypeStruct((ITERS + 1, ITERS), f32),
    )
    anywhere = pl.BlockSpec(memory_space=pl.ANY)
    return pl.pallas_call(
        functools.partial(kernel, slabs, subs, cx, cy, nz),
        out_shape=out_shape,
        in_specs=[pl.BlockSpec(memory_space=pltpu.HBM)] * 4,
        out_specs=(anywhere, anywhere, pl.BlockSpec(memory_space=pltpu.VMEM)),
        scratch_shapes=[
            field(ITERS, cx + 2 * WP),
            field(ITERS, 3, cx + 2 * WU),
            field(ITERS - 1, cx + 2 * WP),
            field(ITERS - 1, 3, cx + 2 * WU),
            field(5, cx + 2 * WC),
            field(9, cx + 2 * WC),
            field(4),
            field(cx + 2 * (WP - 1)),
            field(ITERS, cx + 2 * WQ),
            field(3, cx + 2 * WU),
            field(3, cx + 2),
            pltpu.VMEM((4, cx, cy, nz), f32),
            pltpu.VMEM((ITERS + 1, 4, cx, cy, nz), f32),
            pltpu.VMEM((ITERS, 4, cx, cy, nz), f32),
            pltpu.VMEM((ITERS + 1, n, 1, LANES), f32),
            pltpu.SemaphoreType.DMA((12, 5)),
            pltpu.SemaphoreType.DMA((12, 5)),
            pltpu.SemaphoreType.DMA((ITERS + 1,)),
            pltpu.SemaphoreType.DMA((ITERS + 1,)),
            pltpu.SemaphoreType.DMA((5,)),
            pltpu.SemaphoreType.DMA((2, ITERS + 1)),
        ],
        compiler_params=pltpu.CompilerParams(
            collective_id=0, has_side_effects=True, vmem_limit_bytes=40 * 1024 * 1024
        ),
    )(start, wind, reaction, mass)


def solution(mesh):
    slabs, subs = mesh.shape["slab"], mesh.shape["sub"]
    return jax.shard_map(
        functools.partial(per_device, slabs, subs),
        mesh=mesh,
        in_specs=(
            P(None, "slab", "sub", None),
            P(None, "slab", "sub", None),
            P("slab", "sub", None),
            P("slab", "sub", None),
        ),
        out_specs=(P(None, None, "slab", "sub", None), P(None, None, "slab", "sub", None), P()),
        check_vma=False,
    )
```

```python
import functools

import jax
import jax.numpy as jnp
from jax import lax
from jax.experimental import pallas as pl
from jax.experimental.pallas import tpu as pltpu
from jax.sharding import PartitionSpec as P

ITERS = 3
UNROLL = 3
WP, WU, WC, WQ = 2, 2, 2, 3
HALO = 8
LANES = 128
MESH = pl.DeviceIdType.MESH


def fold(x):
    rows, cols = x.shape
    total = None
    for r in range(0, rows, 8):
        for c in range(0, cols, LANES):
            piece = x[r : r + 8, c : c + LANES]
            total = piece if total is None else total + piece
    return total


def kernel(
    slabs, subs, cx, cy, nz,
    start, wind, reaction, mass, basis, search, hess,
    xp, xu, vp, vu, raw, co, mk, t1, qs, y0, y1, wl, ob, os_, red,
    send, recv, red_send, red_recv, load, store,
):
    slab, sub = lax.axis_index("slab"), lax.axis_index("sub")
    n = slabs * subs
    me = slab * subs + sub
    rows = cy + HALO
    has_left, has_right = slab > 0, slab < slabs - 1

    loads = [
        pltpu.make_async_copy(start.at[3], xp.at[0, pl.ds(WP, cx), pl.ds(0, cy)], load.at[0]),
        pltpu.make_async_copy(
            start.at[pl.ds(0, 3)], xu.at[0, :, pl.ds(WU, cx), pl.ds(0, cy)], load.at[1]
        ),
        pltpu.make_async_copy(
            wind, raw.at[pl.ds(0, 3), pl.ds(WC, cx), pl.ds(0, cy)], load.at[2]
        ),
        pltpu.make_async_copy(reaction, raw.at[3, pl.ds(WC, cx), pl.ds(0, cy)], load.at[3]),
        pltpu.make_async_copy(mass, raw.at[4, pl.ds(WC, cx), pl.ds(0, cy)], load.at[4]),
    ]
    for item in loads:
        item.start()

    barrier = pltpu.get_barrier_semaphore()

    def greet(k, carry):
        for other in range(subs):
            pl.semaphore_signal(
                barrier, inc=1, device_id=(lax.rem(slab + k, slabs), other), device_id_type=MESH
            )
        return carry

    for k in range(1, subs):
        pl.semaphore_signal(
            barrier, inc=1, device_id=(slab, lax.rem(sub + k, subs)), device_id_type=MESH
        )
    lax.fori_loop(1, slabs, greet, 0)

    def clear(low):
        def inner():
            for e in range(ITERS):
                for k in range(WP):
                    at = k if low else WP + cx + k
                    xp[e, at, 0:cy] = jnp.zeros((cy, nz), jnp.float32)
                for k in range(WQ):
                    at = k if low else WQ + cx + k
                    qs[e, at, 0:cy] = jnp.zeros((cy, nz), jnp.float32)
                for c in range(3):
                    for k in range(WU):
                        at = k if low else WU + cx + k
                        xu[e, c, at, 0:cy] = jnp.zeros((cy, nz), jnp.float32)
            for c in range(5):
                for k in range(WC):
                    at = k if low else WC + cx + k
                    raw[c, at, 0:cy] = jnp.zeros((cy, nz), jnp.float32)
        return inner

    pl.when(jnp.logical_not(has_left))(clear(True))
    pl.when(jnp.logical_not(has_right))(clear(False))

    row = lax.broadcasted_iota(jnp.int32, (rows, nz), 0)
    col = lax.broadcasted_iota(jnp.int32, (rows, nz), 1)
    last = jnp.where(sub == 0, rows - 1, cy - 1)
    first = jnp.where(sub == 0, 0, cy)
    mk[0] = jnp.where(row == last, 0.0, 1.0)
    mk[1] = jnp.where(row == first, 0.0, 1.0)
    mk[2] = jnp.where(col == nz - 1, 0.0, 1.0)
    mk[3] = jnp.where(col == 0, 0.0, 1.0)

    pl.semaphore_wait(barrier, n - 1)

    def p_view(e):
        return lambda planes, lines: xp.at[e, planes, lines]

    def u_view(e):
        return lambda planes, lines: xu.at[e, :, planes, lines]

    def q_view(e):
        return lambda planes, lines: qs.at[e, planes, lines]

    def wind_view(planes, lines):
        return raw.at[pl.ds(0, 3), planes, lines]

    def row_view(i):
        return lambda planes, lines: raw.at[i, planes, lines]

    every, across = (0, 1, 2, 3, 4), (0, 1, 3, 4)
    groups = [
        (p_view(0), WP, WP, every), (u_view(0), WU, WU, every),
        (row_view(3), WC, WC, every),
        (p_view(1), WP, WP, every), (u_view(1), WU, WU, every),
        (p_view(2), WP, WP, every), (u_view(2), WU, WU, every),
        (wind_view, WC, 1, every), (row_view(4), WC, 0, (2,)),
        (q_view(0), WQ, WQ, across), (q_view(1), WQ, WQ, across), (q_view(2), WQ, WQ, across),
    ]
    own_lines = pl.ds(0, cy)
    edge_lines = pl.ds(pl.multiple_of((1 - sub) * (cy - HALO), 8), HALO)
    halo_lines = pl.ds(cy, HALO)

    def remote(g, kind):
        view, base, w, _ = groups[g]
        end = base + cx
        if kind == 0:
            src, dst = view(pl.ds(end - w, w), own_lines), view(pl.ds(base - w, w), own_lines)
            target = {"slab": slab + 1}
        elif kind == 1:
            src, dst = view(pl.ds(base, w), own_lines), view(pl.ds(end, w), own_lines)
            target = {"slab": slab - 1}
        else:
            planes = (pl.ds(base, cx), pl.ds(base - w, w), pl.ds(end, w))[kind - 2]
            src, dst = view(planes, edge_lines), view(planes, halo_lines)
            target = {"sub": 1 - sub}
        return pltpu.make_async_remote_copy(
            src_ref=src, dst_ref=dst, send_sem=send.at[g, kind], recv_sem=recv.at[g, kind],
            device_id=target, device_id_type=MESH,
        )

    def begin(g):
        kinds = groups[g][3]
        if 0 in kinds:
            pl.when(has_right)(lambda: remote(g, 0).start())
            pl.when(has_left)(lambda: remote(g, 1).start())
        if 2 in kinds:
            remote(g, 2).start()

    def forward(g):
        if 0 in groups[g][3]:
            pl.when(has_left)(lambda: remote(g, 0).wait_recv())
            remote(g, 3).start()
            pl.when(has_right)(lambda: remote(g, 1).wait_recv())
            remote(g, 4).start()

    def arrive(g, kinds=(2, 3, 4)):
        for kind in groups[g][3]:
            if kind in kinds:
                remote(g, kind).wait_recv()

    def finish(g):
        for kind in groups[g][3]:
            if kind == 0:
                pl.when(has_right)(lambda: remote(g, 0).wait_send())
            elif kind == 1:
                pl.when(has_left)(lambda: remote(g, 1).wait_send())
            else:
                remote(g, kind).wait_send()

    lane = lax.broadcasted_iota(jnp.int32, (1, LANES), 1)

    def reduce_start(e, parts):
        line = jnp.zeros((1, LANES), jnp.float32)
        for i, part in enumerate(parts):
            line = line + jnp.where(lane == i, jnp.sum(fold(part), keepdims=True), 0.0)
        red[e, me] = line

        def tell(at, core):
            pltpu.make_async_remote_copy(
                src_ref=red.at[e, me], dst_ref=red.at[e, me],
                send_sem=red_send.at[e], recv_sem=red_recv.at[e],
                device_id=(at, core), device_id_type=MESH,
            ).start()

        def push(k, carry):
            at = lax.rem(slab + k, slabs)
            for core in range(subs):
                tell(at, core)
            return carry

        lax.fori_loop(1, slabs, push, 0)
        for k in range(1, subs):
            tell(slab, lax.rem(sub + k, subs))

    def red_wait(e, sem):
        block = red.at[e, pl.ds(0, n - 1)]
        pltpu.make_async_copy(block, block, sem.at[e]).wait()

    def reduce_end(e, count):
        red_wait(e, red_recv)
        total = jnp.sum(red[e], axis=0)
        return [
            jnp.sum(jnp.where(lane == i, total, 0.0), axis=1, keepdims=True)
            for i in range(count)
        ]

    def turn(f):
        return (
            pltpu.roll(f, rows - 1, 0), pltpu.roll(f, 1, 0),
            pltpu.roll(f, nz - 1, 1), pltpu.roll(f, 1, 1),
        )

    def masked(f):
        yp, ym, zp, zm = turn(f)
        return yp * mk[0], ym * mk[1], zp * mk[2], zm * mk[3]

    def off_diagonal(below, around, above, k):
        yp, ym, zp, zm = around
        total = co[0, k] * above + co[1, k] * below
        total = total + (co[2, k] * yp + co[3, k] * ym)
        return total + (co[4, k] * zp + co[5, k] * zm)

    def loop(count, body, init=0, low=0):
        step = max(u for u in range(1, UNROLL + 1) if count % u == 0)

        def several(k, carry):
            for i in range(step):
                carry = body(low + k * step + i, carry)
            return carry

        return lax.fori_loop(0, count // step, several, init)

    def spans(spans_of, body):
        for low, high in spans_of:
            if high > low:
                loop(high - low, body, low=low)

    def inside(k, w):
        at = slab * cx + k - w
        return jnp.logical_and(at >= 0, at < slabs * cx)

    def coefficients():
        def body(k, carry):
            ok = jnp.where(inside(k, WC), 1.0, 0.0)
            keep = jnp.full((rows, nz), ok) > 0.5
            hx, hy, hz = 0.5 * raw[0, k], 0.5 * raw[1, k], 0.5 * raw[2, k]
            co[0, k] = 1.0 - hx
            co[1, k] = 1.0 + hx
            co[2, k] = (1.0 - hy) * mk[0]
            co[3, k] = (1.0 + hy) * mk[1]
            co[4, k] = (1.0 - hz) * mk[2]
            co[5, k] = (1.0 + hz) * mk[3]
            diagonal = 6.0 + raw[3, k]
            co[6, k] = diagonal
            co[7, k] = jnp.where(keep, 1.0 / diagonal, 0.0)
            co[8, k] = jnp.where(keep, 1.0 / raw[4, k], 0.0)
            return carry

        loop(cx + 2 * WC, body)

    def first_guess(p):
        def body(k, carry):
            here = p[k + 1]
            yp, ym, zp, zm = masked(here)
            total = (p[k] + p[k + 2]) + (yp + ym) + (zp + zm)
            ok = jnp.where(inside(k, WP - 1), 1.0 / 7.0, 0.0)
            t1[k] = (here + total * (1.0 / 7.0)) * ok
            return carry

        loop(cx + 2 * (WP - 1), body)

    def schur(qq):
        def body(k, carry):
            here = t1[k + 1]
            off = off_diagonal(t1[k], turn(here), t1[k + 2], k + WC)
            qq[k + WQ] = (off - co[6, k + WC] * here) * co[8, k + WC]
            return carry

        loop(cx, body)

    def velocity_first(qq, u, where):
        def body(k, carry):
            yp, ym, zp, zm = masked(qq[k + 1])
            scale = co[7, k]
            y0[0, k] = (u[0, k] - 0.5 * (qq[k + 2] - qq[k])) * scale
            y0[1, k] = (u[1, k] - 0.5 * (yp - ym)) * scale
            y0[2, k] = (u[2, k] - 0.5 * (zp - zm)) * scale
            return carry

        spans(where, body)

    def velocity_second(where):
        def body(k, carry):
            scale = co[7, k + 1]
            for c in range(3):
                here = y0[c, k + 1]
                off = off_diagonal(y0[c, k], turn(here), y0[c, k + 2], k + 1)
                y1[c, k] = here + off * scale
            return carry

        spans(where, body)

    def image(e, qq, vectors):
        def body(k, acc):
            q = qq[k + WQ]
            qa, qb = qq[k + WQ + 1], qq[k + WQ - 1]
            yp, ym, zp, zm = masked(q)
            grads = (0.5 * (qa - qb), 0.5 * (yp - ym), 0.5 * (zp - zm))
            low = 0.5 * ((qa + qb) + (yp + ym) + (zp + zm)) - 3.0 * q
            out = []
            for c in range(3):
                here = y1[c, k + 1]
                below, above = y1[c, k], y1[c, k + 2]
                around = turn(here)
                off = off_diagonal(below, around, above, k + WC)
                w = (co[6, k + WC] * here - off + grads[c])[:cy]
                if c == 0:
                    low = low - 0.5 * (above - below)
                elif c == 1:
                    low = low - 0.5 * (around[0] * mk[0] - around[1] * mk[1])
                else:
                    low = low - 0.5 * (around[2] * mk[2] - around[3] * mk[3])
                os_[e, c, k] = here[:cy]
                out.append(w)
            os_[e, 3, k] = q[:cy]
            out.append(low[:cy])
            if e + 1 < ITERS:
                for c in range(3):
                    xu[e + 1, c, k + WU, 0:cy] = out[c]
                xp[e + 1, k + WP, 0:cy] = out[3]
            else:
                for c in range(4):
                    wl[c, k] = out[c]
            acc = list(acc)
            for i, (p, u) in enumerate(vectors):
                held = [u[c, k + WU, 0:cy] for c in range(3)] + [p[k + WP, 0:cy]]
                term = held[0] * out[0] + held[1] * out[1]
                acc[i + 1] = acc[i + 1] + (term + (held[2] * out[2] + held[3] * out[3]))
                if i == e:
                    term = held[0] * held[0] + held[1] * held[1]
                    acc[0] = acc[0] + (term + (held[2] * held[2] + held[3] * held[3]))
            return tuple(acc)

        zero = jnp.zeros((cy, nz), jnp.float32)
        return loop(cx, body, (zero,) * (e + 2))

    def write_out(e):
        return (
            pltpu.make_async_copy(ob.at[e], basis.at[e], store.at[0, e]),
            pltpu.make_async_copy(os_.at[e], search.at[e], store.at[1, e]),
        )

    def results(e, vector, inverse):
        p, u = vector

        def body(k, carry):
            for c in range(3):
                ob[e, c, k] = u[c, k + WU, 0:cy] * inverse
            ob[e, 3, k] = p[k + WP, 0:cy] * inverse
            for c in range(4):
                os_[e, c, k] = os_[e, c, k] * inverse
            return carry

        loop(cx, body)
        for item in write_out(e):
            item.start()

    loads[0].wait()
    begin(0)
    for item in loads[2:]:
        item.wait()
    for g in (2, 7, 8):
        begin(g)
    loads[1].wait()
    begin(1)
    forward(0)
    arrive(0)

    vectors = [(xp.at[0], xu.at[0])]
    inverses = []
    entries = {}
    first_guess(vectors[0][0])
    for g in (2, 7):
        forward(g)
    for g in (2, 7, 8):
        arrive(g)
    coefficients()
    for e in range(ITERS):
        p, u = vectors[e]
        p_group, u_group = ((0, 1), (3, 4), (5, 6))[e]
        if e > 0:
            first_guess(p)
        qq = qs.at[e]
        schur(qq)
        begin(9 + e)
        if e > 0:
            results(e - 1, vectors[e - 1], inverses[e - 1])
        end_u, end_1 = cx + 2 * WU, cx + 2
        deep = min(3, end_1 // 2)
        inner = (WU + 1, WU + cx - 1)
        arrive(u_group, (2,))
        if e > 0:

            def form_u(k, carry, e=e):
                for c in range(3):
                    total = xu[e, c, k] * factor
                    for g, (_, other) in zip(weights, vectors[:e]):
                        total = total - g * other[c, k]
                    u[c, k] = total
                return carry

            spans([(WU, WU + cx)], form_u)
        velocity_first(qq, u, [inner])
        velocity_second([(deep, end_1 - deep)])
        forward(u_group)
        forward(9 + e)
        arrive(u_group, (3, 4))
        if e > 0:
            spans([(0, WU), (WU + cx, end_u)], form_u)
        arrive(9 + e)
        velocity_first(qq, u, [(0, inner[0]), (inner[1], end_u)])
        velocity_second([(0, deep), (end_1 - deep, end_1)])
        acc = image(e, qq, vectors)
        reduce_start(e, acc)
        if e + 1 < ITERS:
            begin(p_group + 3 if e == 0 else 5)
            begin(u_group + 3 if e == 0 else 6)
        sums = reduce_end(e, e + 2)
        norm = jnp.sqrt(sums[0])
        factor = 1.0 / norm
        if e > 0:
            entries[(e, e - 1)] = norm
        inverses.append(factor)
        weights = []
        for i in range(e + 1):
            h = sums[i + 1] * inverses[i] * factor
            entries[(i, e)] = h
            weights.append(h * inverses[i])
        if e + 1 < ITERS:
            g_p = (3, 5)[e]
            forward(g_p)
            arrive(g_p)
            new = (vp.at[e], vu.at[e])

            def form_p(k, carry, e=e):
                total = xp[e + 1, k] * factor
                for g, (other, _) in zip(weights, vectors[: e + 1]):
                    total = total - g * other[k]
                vp[e, k] = total
                return carry

            loop(cx + 2 * WP, form_p)
            vectors.append(new)

    def close(k, acc):
        for c in range(4):
            total = wl[c, k] * factor
            for g, (p, u) in zip(weights, vectors):
                held = p[k + WP, 0:cy] if c == 3 else u[c, k + WU, 0:cy]
                total = total - g * held
            ob[ITERS, c, k] = total
            acc = acc + total * total
        return acc

    acc = loop(cx, close, jnp.zeros((cy, nz), jnp.float32))
    reduce_start(ITERS, [acc])
    results(ITERS - 1, vectors[ITERS - 1], inverses[ITERS - 1])
    for g in range(len(groups)):
        finish(g)
    norm = jnp.sqrt(reduce_end(ITERS, 1)[0])
    entries[(ITERS, ITERS - 1)] = norm
    factor = 1.0 / norm

    def scale(k, carry):
        for c in range(4):
            ob[ITERS, c, k] = ob[ITERS, c, k] * factor
        return carry

    loop(cx, scale)
    final = pltpu.make_async_copy(ob.at[ITERS], basis.at[ITERS], store.at[0, ITERS])
    final.start()
    r = lax.broadcasted_iota(jnp.int32, (ITERS + 1, ITERS), 0)
    c = lax.broadcasted_iota(jnp.int32, (ITERS + 1, ITERS), 1)
    table = jnp.zeros((ITERS + 1, ITERS), jnp.float32)
    for (i, j), value in entries.items():
        table = table + jnp.where(jnp.logical_and(r == i, c == j), value, 0.0)
    hess[...] = table
    for e in range(ITERS + 1):
        red_wait(e, red_send)
    for e in range(ITERS):
        for item in write_out(e):
            item.wait()
    final.wait()


def per_device(slabs, subs, start, wind, reaction, mass):
    _, cx, cy, nz = start.shape
    n = slabs * subs
    rows = cy + HALO
    f32 = jnp.float32

    def field(*lead):
        return pltpu.VMEM((*lead, rows, nz), f32)

    out_shape = (
        jax.ShapeDtypeStruct((ITERS + 1, 4, cx, cy, nz), f32),
        jax.ShapeDtypeStruct((ITERS, 4, cx, cy, nz), f32),
        jax.ShapeDtypeStruct((ITERS + 1, ITERS), f32),
    )
    anywhere = pl.BlockSpec(memory_space=pl.ANY)
    return pl.pallas_call(
        functools.partial(kernel, slabs, subs, cx, cy, nz),
        out_shape=out_shape,
        in_specs=[pl.BlockSpec(memory_space=pltpu.HBM)] * 4,
        out_specs=(anywhere, anywhere, pl.BlockSpec(memory_space=pltpu.VMEM)),
        scratch_shapes=[
            field(ITERS, cx + 2 * WP),
            field(ITERS, 3, cx + 2 * WU),
            field(ITERS - 1, cx + 2 * WP),
            field(ITERS - 1, 3, cx + 2 * WU),
            field(5, cx + 2 * WC),
            field(9, cx + 2 * WC),
            field(4),
            field(cx + 2 * (WP - 1)),
            field(ITERS, cx + 2 * WQ),
            field(3, cx + 2 * WU),
            field(3, cx + 2),
            pltpu.VMEM((4, cx, cy, nz), f32),
            pltpu.VMEM((ITERS + 1, 4, cx, cy, nz), f32),
            pltpu.VMEM((ITERS, 4, cx, cy, nz), f32),
            pltpu.VMEM((ITERS + 1, n, 1, LANES), f32),
            pltpu.SemaphoreType.DMA((12, 5)),
            pltpu.SemaphoreType.DMA((12, 5)),
            pltpu.SemaphoreType.DMA((ITERS + 1,)),
            pltpu.SemaphoreType.DMA((ITERS + 1,)),
            pltpu.SemaphoreType.DMA((5,)),
            pltpu.SemaphoreType.DMA((2, ITERS + 1)),
        ],
        compiler_params=pltpu.CompilerParams(
            collective_id=0, has_side_effects=True, vmem_limit_bytes=63_900_000
        ),
    )(start, wind, reaction, mass)


def solution(mesh):
    slabs, subs = mesh.shape["slab"], mesh.shape["sub"]
    return jax.shard_map(
        functools.partial(per_device, slabs, subs),
        mesh=mesh,
        in_specs=(
            P(None, "slab", "sub", None),
            P(None, "slab", "sub", None),
            P("slab", "sub", None),
            P("slab", "sub", None),
        ),
        out_specs=(P(None, None, "slab", "sub", None), P(None, None, "slab", "sub", None), P()),
        check_vma=False,
    )
```

```python
import functools

import jax
import jax.numpy as jnp
from jax import lax
from jax.experimental import pallas as pl
from jax.experimental.pallas import tpu as pltpu
from jax.sharding import PartitionSpec as P

ITERS = 3
UNROLL = 3
WP, WU, WC, WQ = 2, 2, 2, 3
HALO = 8
LANES = 128
MESH = pl.DeviceIdType.MESH


def fold(x):
    rows, cols = x.shape
    total = None
    for r in range(0, rows, 8):
        for c in range(0, cols, LANES):
            piece = x[r : r + 8, c : c + LANES]
            total = piece if total is None else total + piece
    return total


def kernel(
    slabs, subs, cx, cy, nz,
    start, wind, reaction, mass, basis, search, hess,
    xp, xu, vp, vu, raw, co, mk, t1, qs, y0, y1, wl, ob, os_, red,
    send, recv, red_send, red_recv, load, store,
):
    slab, sub = lax.axis_index("slab"), lax.axis_index("sub")
    n = slabs * subs
    me = slab * subs + sub
    rows = cy + HALO
    has_left, has_right = slab > 0, slab < slabs - 1

    loads = [
        pltpu.make_async_copy(start.at[3], xp.at[0, pl.ds(WP, cx), pl.ds(0, cy)], load.at[0]),
        pltpu.make_async_copy(
            start.at[pl.ds(0, 3)], xu.at[0, :, pl.ds(WU, cx), pl.ds(0, cy)], load.at[1]
        ),
        pltpu.make_async_copy(
            wind, raw.at[pl.ds(0, 3), pl.ds(WC, cx), pl.ds(0, cy)], load.at[2]
        ),
        pltpu.make_async_copy(reaction, raw.at[3, pl.ds(WC, cx), pl.ds(0, cy)], load.at[3]),
        pltpu.make_async_copy(mass, raw.at[4, pl.ds(WC, cx), pl.ds(0, cy)], load.at[4]),
    ]
    for item in loads:
        item.start()

    barrier = pltpu.get_barrier_semaphore()

    def greet(k, carry):
        for other in range(subs):
            pl.semaphore_signal(
                barrier, inc=1, device_id=(lax.rem(slab + k, slabs), other), device_id_type=MESH
            )
        return carry

    for k in range(1, subs):
        pl.semaphore_signal(
            barrier, inc=1, device_id=(slab, lax.rem(sub + k, subs)), device_id_type=MESH
        )
    lax.fori_loop(1, slabs, greet, 0)

    def clear(low):
        def inner():
            for e in range(ITERS):
                for k in range(WP):
                    at = k if low else WP + cx + k
                    xp[e, at, 0:cy] = jnp.zeros((cy, nz), jnp.float32)
                for k in range(WQ):
                    at = k if low else WQ + cx + k
                    qs[e, at, 0:cy] = jnp.zeros((cy, nz), jnp.float32)
                for c in range(3):
                    for k in range(WU):
                        at = k if low else WU + cx + k
                        xu[e, c, at, 0:cy] = jnp.zeros((cy, nz), jnp.float32)
            for c in range(5):
                for k in range(WC):
                    at = k if low else WC + cx + k
                    raw[c, at, 0:cy] = jnp.zeros((cy, nz), jnp.float32)
        return inner

    pl.when(jnp.logical_not(has_left))(clear(True))
    pl.when(jnp.logical_not(has_right))(clear(False))

    row = lax.broadcasted_iota(jnp.int32, (rows, nz), 0)
    col = lax.broadcasted_iota(jnp.int32, (rows, nz), 1)
    last = jnp.where(sub == 0, rows - 1, cy - 1)
    first = jnp.where(sub == 0, 0, cy)
    mk[0] = jnp.where(row == last, 0.0, 1.0)
    mk[1] = jnp.where(row == first, 0.0, 1.0)
    mk[2] = jnp.where(col == nz - 1, 0.0, 1.0)
    mk[3] = jnp.where(col == 0, 0.0, 1.0)

    pl.semaphore_wait(barrier, n - 1)

    def p_view(e):
        return lambda planes, lines: xp.at[e, planes, lines]

    def u_view(e):
        return lambda planes, lines: xu.at[e, :, planes, lines]

    def q_view(e):
        return lambda planes, lines: qs.at[e, planes, lines]

    def wind_view(planes, lines):
        return raw.at[pl.ds(0, 3), planes, lines]

    def row_view(i):
        return lambda planes, lines: raw.at[i, planes, lines]

    every, across = (0, 1, 2, 3, 4), (0, 1, 3, 4)
    groups = [
        (p_view(0), WP, WP, every), (u_view(0), WU, WU, every),
        (row_view(3), WC, WC, every),
        (p_view(1), WP, WP, every), (u_view(1), WU, WU, every),
        (p_view(2), WP, WP, every), (u_view(2), WU, WU, every),
        (wind_view, WC, 1, every), (row_view(4), WC, 0, (2,)),
        (q_view(0), WQ, WQ, across), (q_view(1), WQ, WQ, across), (q_view(2), WQ, WQ, across),
    ]
    own_lines = pl.ds(0, cy)
    edge_lines = pl.ds(pl.multiple_of((1 - sub) * (cy - HALO), 8), HALO)
    halo_lines = pl.ds(cy, HALO)

    def remote(g, kind):
        view, base, w, _ = groups[g]
        end = base + cx
        if kind == 0:
            src, dst = view(pl.ds(end - w, w), own_lines), view(pl.ds(base - w, w), own_lines)
            target = {"slab": slab + 1}
        elif kind == 1:
            src, dst = view(pl.ds(base, w), own_lines), view(pl.ds(end, w), own_lines)
            target = {"slab": slab - 1}
        else:
            planes = (pl.ds(base, cx), pl.ds(base - w, w), pl.ds(end, w))[kind - 2]
            src, dst = view(planes, edge_lines), view(planes, halo_lines)
            target = {"sub": 1 - sub}
        return pltpu.make_async_remote_copy(
            src_ref=src, dst_ref=dst, send_sem=send.at[g, kind], recv_sem=recv.at[g, kind],
            device_id=target, device_id_type=MESH,
        )

    def begin(g, chosen=(0, 1, 2)):
        kinds = [kind for kind in groups[g][3] if kind in chosen]
        if 0 in kinds:
            pl.when(has_right)(lambda: remote(g, 0).start())
            pl.when(has_left)(lambda: remote(g, 1).start())
        if 2 in kinds:
            remote(g, 2).start()

    def forward(g):
        if 0 in groups[g][3]:
            pl.when(has_left)(lambda: remote(g, 0).wait_recv())
            remote(g, 3).start()
            pl.when(has_right)(lambda: remote(g, 1).wait_recv())
            remote(g, 4).start()

    def arrive(g, kinds=(2, 3, 4)):
        for kind in groups[g][3]:
            if kind in kinds:
                remote(g, kind).wait_recv()

    def finish(g):
        for kind in groups[g][3]:
            if kind == 0:
                pl.when(has_right)(lambda: remote(g, 0).wait_send())
            elif kind == 1:
                pl.when(has_left)(lambda: remote(g, 1).wait_send())
            else:
                remote(g, kind).wait_send()

    lane = lax.broadcasted_iota(jnp.int32, (1, LANES), 1)

    def reduce_start(e, parts):
        line = jnp.zeros((1, LANES), jnp.float32)
        for i, part in enumerate(parts):
            line = line + jnp.where(lane == i, jnp.sum(fold(part), keepdims=True), 0.0)
        red[e, me] = line

        def tell(at, core):
            pltpu.make_async_remote_copy(
                src_ref=red.at[e, me], dst_ref=red.at[e, me],
                send_sem=red_send.at[e], recv_sem=red_recv.at[e],
                device_id=(at, core), device_id_type=MESH,
            ).start()

        def push(k, carry):
            at = lax.rem(slab + k, slabs)
            for core in range(subs):
                tell(at, core)
            return carry

        lax.fori_loop(1, slabs, push, 0)
        for k in range(1, subs):
            tell(slab, lax.rem(sub + k, subs))

    def red_wait(e, sem):
        block = red.at[e, pl.ds(0, n - 1)]
        pltpu.make_async_copy(block, block, sem.at[e]).wait()

    def reduce_end(e, count):
        red_wait(e, red_recv)
        total = jnp.sum(red[e], axis=0)
        return [
            jnp.sum(jnp.where(lane == i, total, 0.0), axis=1, keepdims=True)
            for i in range(count)
        ]

    def turn(f):
        return (
            pltpu.roll(f, rows - 1, 0), pltpu.roll(f, 1, 0),
            pltpu.roll(f, nz - 1, 1), pltpu.roll(f, 1, 1),
        )

    def masked(f):
        yp, ym, zp, zm = turn(f)
        return yp * mk[0], ym * mk[1], zp * mk[2], zm * mk[3]

    def off_diagonal(below, around, above, k):
        yp, ym, zp, zm = around
        total = co[0, k] * above + co[1, k] * below
        total = total + (co[2, k] * yp + co[3, k] * ym)
        return total + (co[4, k] * zp + co[5, k] * zm)

    def loop(count, body, init=0, low=0):
        step = max(u for u in range(1, UNROLL + 1) if count % u == 0)

        def several(k, carry):
            for i in range(step):
                carry = body(low + k * step + i, carry)
            return carry

        return lax.fori_loop(0, count // step, several, init)

    def spans(spans_of, body):
        for low, high in spans_of:
            if high > low:
                loop(high - low, body, low=low)

    def inside(k, w):
        at = slab * cx + k - w
        return jnp.logical_and(at >= 0, at < slabs * cx)

    def coefficients(where):
        def body(k, carry):
            ok = jnp.where(inside(k, WC), 1.0, 0.0)
            keep = jnp.full((rows, nz), ok) > 0.5
            hx, hy, hz = 0.5 * raw[0, k], 0.5 * raw[1, k], 0.5 * raw[2, k]
            co[0, k] = 1.0 - hx
            co[1, k] = 1.0 + hx
            co[2, k] = (1.0 - hy) * mk[0]
            co[3, k] = (1.0 + hy) * mk[1]
            co[4, k] = (1.0 - hz) * mk[2]
            co[5, k] = (1.0 + hz) * mk[3]
            diagonal = 6.0 + raw[3, k]
            co[6, k] = diagonal
            co[7, k] = jnp.where(keep, 1.0 / diagonal, 0.0)
            co[8, k] = jnp.where(keep, 1.0 / raw[4, k], 0.0)
            return carry

        spans(where, body)

    def first_guess(p):
        def body(k, carry):
            here = p[k + 1]
            yp, ym, zp, zm = masked(here)
            total = (p[k] + p[k + 2]) + (yp + ym) + (zp + zm)
            ok = jnp.where(inside(k, WP - 1), 1.0 / 7.0, 0.0)
            t1[k] = (here + total * (1.0 / 7.0)) * ok
            return carry

        loop(cx + 2 * (WP - 1), body)

    def schur(qq):
        def body(k, carry):
            here = t1[k + 1]
            off = off_diagonal(t1[k], turn(here), t1[k + 2], k + WC)
            qq[k + WQ] = (off - co[6, k + WC] * here) * co[8, k + WC]
            return carry

        loop(cx, body)

    def velocity_first(qq, u, where):
        def body(k, carry):
            yp, ym, zp, zm = masked(qq[k + 1])
            scale = co[7, k]
            y0[0, k] = (u[0, k] - 0.5 * (qq[k + 2] - qq[k])) * scale
            y0[1, k] = (u[1, k] - 0.5 * (yp - ym)) * scale
            y0[2, k] = (u[2, k] - 0.5 * (zp - zm)) * scale
            return carry

        spans(where, body)

    def velocity_second(where):
        def body(k, carry):
            scale = co[7, k + 1]
            for c in range(3):
                here = y0[c, k + 1]
                off = off_diagonal(y0[c, k], turn(here), y0[c, k + 2], k + 1)
                y1[c, k] = here + off * scale
            return carry

        spans(where, body)

    def image(e, qq, vectors):
        def body(k, acc):
            q = qq[k + WQ]
            qa, qb = qq[k + WQ + 1], qq[k + WQ - 1]
            yp, ym, zp, zm = masked(q)
            grads = (0.5 * (qa - qb), 0.5 * (yp - ym), 0.5 * (zp - zm))
            low = 0.5 * ((qa + qb) + (yp + ym) + (zp + zm)) - 3.0 * q
            out = []
            for c in range(3):
                here = y1[c, k + 1]
                below, above = y1[c, k], y1[c, k + 2]
                around = turn(here)
                off = off_diagonal(below, around, above, k + WC)
                w = (co[6, k + WC] * here - off + grads[c])[:cy]
                if c == 0:
                    low = low - 0.5 * (above - below)
                elif c == 1:
                    low = low - 0.5 * (around[0] * mk[0] - around[1] * mk[1])
                else:
                    low = low - 0.5 * (around[2] * mk[2] - around[3] * mk[3])
                os_[e, c, k] = here[:cy]
                out.append(w)
            os_[e, 3, k] = q[:cy]
            out.append(low[:cy])
            if e + 1 < ITERS:
                for c in range(3):
                    xu[e + 1, c, k + WU, 0:cy] = out[c]
                xp[e + 1, k + WP, 0:cy] = out[3]
            else:
                for c in range(4):
                    wl[c, k] = out[c]
            acc = list(acc)
            for i, (p, u) in enumerate(vectors):
                held = [u[c, k + WU, 0:cy] for c in range(3)] + [p[k + WP, 0:cy]]
                term = held[0] * out[0] + held[1] * out[1]
                acc[i + 1] = acc[i + 1] + (term + (held[2] * out[2] + held[3] * out[3]))
                if i == e:
                    term = held[0] * held[0] + held[1] * held[1]
                    acc[0] = acc[0] + (term + (held[2] * held[2] + held[3] * held[3]))
            return tuple(acc)

        zero = jnp.zeros((cy, nz), jnp.float32)
        acc = (zero,) * (e + 2)
        acc = loop(WP, body, acc)
        acc = loop(WP, body, acc, low=cx - WP)
        if e + 1 < ITERS:
            begin((3, 5)[e], (0, 1))
        acc = loop(cx - 2 * WP, body, acc, low=WP)
        if e + 1 < ITERS:
            begin((3, 5)[e], (2,))
        return acc

    def write_out(e):
        return (
            pltpu.make_async_copy(ob.at[e], basis.at[e], store.at[0, e]),
            pltpu.make_async_copy(os_.at[e], search.at[e], store.at[1, e]),
        )

    def results(e, vector, inverse):
        p, u = vector

        def body(k, carry):
            for c in range(3):
                ob[e, c, k] = u[c, k + WU, 0:cy] * inverse
            ob[e, 3, k] = p[k + WP, 0:cy] * inverse
            for c in range(4):
                os_[e, c, k] = os_[e, c, k] * inverse
            return carry

        loop(cx, body)
        for item in write_out(e):
            item.start()

    loads[0].wait()
    begin(0)
    for item in loads[2:]:
        item.wait()
    for g in (2, 7, 8):
        begin(g, (2,))
    loads[1].wait()
    begin(1)
    for g in (2, 7):
        begin(g, (0, 1))
    for g in (2, 7, 8):
        arrive(g, (2,))
    coefficients([(WC, WC + cx)])
    forward(0)
    arrive(0)

    vectors = [(xp.at[0], xu.at[0])]
    inverses = []
    entries = {}
    first_guess(vectors[0][0])
    for e in range(ITERS):
        p, u = vectors[e]
        p_group, u_group = ((0, 1), (3, 4), (5, 6))[e]
        if e > 0:
            first_guess(p)
        qq = qs.at[e]
        schur(qq)
        begin(9 + e)
        if e > 0:
            results(e - 1, vectors[e - 1], inverses[e - 1])
        end_u, end_1 = cx + 2 * WU, cx + 2
        deep = min(3, end_1 // 2)
        inner = (WU + 1, WU + cx - 1)
        arrive(u_group, (2,))
        if e > 0:

            def form_u(k, carry, e=e):
                for c in range(3):
                    total = xu[e, c, k] * factor
                    for g, (_, other) in zip(weights, vectors[:e]):
                        total = total - g * other[c, k]
                    u[c, k] = total
                return carry

            spans([(WU, WU + cx)], form_u)
        velocity_first(qq, u, [inner])
        velocity_second([(deep, end_1 - deep)])
        forward(u_group)
        if e == 0:
            for g in (2, 7):
                forward(g)
            for g in (2, 7):
                arrive(g, (3, 4))
            coefficients([(0, WC), (WC + cx, cx + 2 * WC)])
        forward(9 + e)
        arrive(u_group, (3, 4))
        if e > 0:
            spans([(0, WU), (WU + cx, end_u)], form_u)
        arrive(9 + e)
        velocity_first(qq, u, [(0, inner[0]), (inner[1], end_u)])
        velocity_second([(0, deep), (end_1 - deep, end_1)])
        acc = image(e, qq, vectors)
        reduce_start(e, acc)
        if e + 1 < ITERS:
            begin(u_group + 3 if e == 0 else 6)
        sums = reduce_end(e, e + 2)
        norm = jnp.sqrt(sums[0])
        factor = 1.0 / norm
        if e > 0:
            entries[(e, e - 1)] = norm
        inverses.append(factor)
        weights = []
        for i in range(e + 1):
            h = sums[i + 1] * inverses[i] * factor
            entries[(i, e)] = h
            weights.append(h * inverses[i])
        if e + 1 < ITERS:
            g_p = (3, 5)[e]
            forward(g_p)
            arrive(g_p)
            new = (vp.at[e], vu.at[e])

            def form_p(k, carry, e=e):
                total = xp[e + 1, k] * factor
                for g, (other, _) in zip(weights, vectors[: e + 1]):
                    total = total - g * other[k]
                vp[e, k] = total
                return carry

            loop(cx + 2 * WP, form_p)
            vectors.append(new)

    def close(k, acc):
        for c in range(4):
            total = wl[c, k] * factor
            for g, (p, u) in zip(weights, vectors):
                held = p[k + WP, 0:cy] if c == 3 else u[c, k + WU, 0:cy]
                total = total - g * held
            ob[ITERS, c, k] = total
            acc = acc + total * total
        return acc

    acc = loop(cx, close, jnp.zeros((cy, nz), jnp.float32))
    reduce_start(ITERS, [acc])
    results(ITERS - 1, vectors[ITERS - 1], inverses[ITERS - 1])
    for g in range(len(groups)):
        finish(g)
    norm = jnp.sqrt(reduce_end(ITERS, 1)[0])
    entries[(ITERS, ITERS - 1)] = norm
    factor = 1.0 / norm

    def scale(k, carry):
        for c in range(4):
            ob[ITERS, c, k] = ob[ITERS, c, k] * factor
        return carry

    loop(cx, scale)
    final = pltpu.make_async_copy(ob.at[ITERS], basis.at[ITERS], store.at[0, ITERS])
    final.start()
    r = lax.broadcasted_iota(jnp.int32, (ITERS + 1, ITERS), 0)
    c = lax.broadcasted_iota(jnp.int32, (ITERS + 1, ITERS), 1)
    table = jnp.zeros((ITERS + 1, ITERS), jnp.float32)
    for (i, j), value in entries.items():
        table = table + jnp.where(jnp.logical_and(r == i, c == j), value, 0.0)
    hess[...] = table
    for e in range(ITERS + 1):
        red_wait(e, red_send)
    for e in range(ITERS):
        for item in write_out(e):
            item.wait()
    final.wait()


def per_device(slabs, subs, start, wind, reaction, mass):
    _, cx, cy, nz = start.shape
    n = slabs * subs
    rows = cy + HALO
    f32 = jnp.float32

    def field(*lead):
        return pltpu.VMEM((*lead, rows, nz), f32)

    out_shape = (
        jax.ShapeDtypeStruct((ITERS + 1, 4, cx, cy, nz), f32),
        jax.ShapeDtypeStruct((ITERS, 4, cx, cy, nz), f32),
        jax.ShapeDtypeStruct((ITERS + 1, ITERS), f32),
    )
    anywhere = pl.BlockSpec(memory_space=pl.ANY)
    return pl.pallas_call(
        functools.partial(kernel, slabs, subs, cx, cy, nz),
        out_shape=out_shape,
        in_specs=[pl.BlockSpec(memory_space=pltpu.HBM)] * 4,
        out_specs=(anywhere, anywhere, pl.BlockSpec(memory_space=pltpu.VMEM)),
        scratch_shapes=[
            field(ITERS, cx + 2 * WP),
            field(ITERS, 3, cx + 2 * WU),
            field(ITERS - 1, cx + 2 * WP),
            field(ITERS - 1, 3, cx + 2 * WU),
            field(5, cx + 2 * WC),
            field(9, cx + 2 * WC),
            field(4),
            field(cx + 2 * (WP - 1)),
            field(ITERS, cx + 2 * WQ),
            field(3, cx + 2 * WU),
            field(3, cx + 2),
            pltpu.VMEM((4, cx, cy, nz), f32),
            pltpu.VMEM((ITERS + 1, 4, cx, cy, nz), f32),
            pltpu.VMEM((ITERS, 4, cx, cy, nz), f32),
            pltpu.VMEM((ITERS + 1, n, 1, LANES), f32),
            pltpu.SemaphoreType.DMA((12, 5)),
            pltpu.SemaphoreType.DMA((12, 5)),
            pltpu.SemaphoreType.DMA((ITERS + 1,)),
            pltpu.SemaphoreType.DMA((ITERS + 1,)),
            pltpu.SemaphoreType.DMA((5,)),
            pltpu.SemaphoreType.DMA((2, ITERS + 1)),
        ],
        compiler_params=pltpu.CompilerParams(
            collective_id=0, has_side_effects=True, vmem_limit_bytes=63_900_000
        ),
    )(start, wind, reaction, mass)


def solution(mesh):
    slabs, subs = mesh.shape["slab"], mesh.shape["sub"]
    return jax.shard_map(
        functools.partial(per_device, slabs, subs),
        mesh=mesh,
        in_specs=(
            P(None, "slab", "sub", None),
            P(None, "slab", "sub", None),
            P("slab", "sub", None),
            P("slab", "sub", None),
        ),
        out_specs=(P(None, None, "slab", "sub", None), P(None, None, "slab", "sub", None), P()),
        check_vma=False,
    )
```

```python
import functools

import jax
import jax.numpy as jnp
from jax import lax
from jax.experimental import pallas as pl
from jax.experimental.pallas import tpu as pltpu
from jax.sharding import PartitionSpec as P

ITERS = 3
UNROLL = 5
WP, WU, WC, WQ = 2, 2, 2, 3
HALO = 8
LANES = 128
MESH = pl.DeviceIdType.MESH


def fold(x):
    rows, cols = x.shape
    total = None
    for r in range(0, rows, 8):
        for c in range(0, cols, LANES):
            piece = x[r : r + 8, c : c + LANES]
            total = piece if total is None else total + piece
    return total


def kernel(
    slabs, subs, cx, cy, nz,
    start, wind, reaction, mass, basis, search, hess,
    xp, xu, vp, vu, raw, co, mk, t1, qs, y0, y1, wl, ob, os_, red,
    send, recv, red_send, red_recv, load, store,
):
    slab, sub = lax.axis_index("slab"), lax.axis_index("sub")
    n = slabs * subs
    me = slab * subs + sub
    rows = cy + HALO
    has_left, has_right = slab > 0, slab < slabs - 1

    loads = [
        pltpu.make_async_copy(start.at[3], xp.at[0, pl.ds(WP, cx), pl.ds(0, cy)], load.at[0]),
        pltpu.make_async_copy(
            start.at[pl.ds(0, 3)], xu.at[0, :, pl.ds(WU, cx), pl.ds(0, cy)], load.at[1]
        ),
        pltpu.make_async_copy(
            wind, raw.at[pl.ds(0, 3), pl.ds(WC, cx), pl.ds(0, cy)], load.at[2]
        ),
        pltpu.make_async_copy(reaction, raw.at[3, pl.ds(WC, cx), pl.ds(0, cy)], load.at[3]),
        pltpu.make_async_copy(mass, raw.at[4, pl.ds(WC, cx), pl.ds(0, cy)], load.at[4]),
    ]
    for item in loads:
        item.start()

    barrier = pltpu.get_barrier_semaphore()

    def greet(k, carry):
        for other in range(subs):
            pl.semaphore_signal(
                barrier, inc=1, device_id=(lax.rem(slab + k, slabs), other), device_id_type=MESH
            )
        return carry

    for k in range(1, subs):
        pl.semaphore_signal(
            barrier, inc=1, device_id=(slab, lax.rem(sub + k, subs)), device_id_type=MESH
        )
    lax.fori_loop(1, slabs, greet, 0)

    def clear(low):
        def inner():
            for e in range(ITERS):
                for k in range(WP):
                    at = k if low else WP + cx + k
                    xp[e, at, 0:cy] = jnp.zeros((cy, nz), jnp.float32)
                for k in range(WQ):
                    at = k if low else WQ + cx + k
                    qs[e, at, 0:cy] = jnp.zeros((cy, nz), jnp.float32)
                for c in range(3):
                    for k in range(WU):
                        at = k if low else WU + cx + k
                        xu[e, c, at, 0:cy] = jnp.zeros((cy, nz), jnp.float32)
            for c in range(5):
                for k in range(WC):
                    at = k if low else WC + cx + k
                    raw[c, at, 0:cy] = jnp.zeros((cy, nz), jnp.float32)
        return inner

    pl.when(jnp.logical_not(has_left))(clear(True))
    pl.when(jnp.logical_not(has_right))(clear(False))

    row = lax.broadcasted_iota(jnp.int32, (rows, nz), 0)
    col = lax.broadcasted_iota(jnp.int32, (rows, nz), 1)
    last = jnp.where(sub == 0, rows - 1, cy - 1)
    first = jnp.where(sub == 0, 0, cy)
    mk[0] = jnp.where(row == last, 0.0, 1.0)
    mk[1] = jnp.where(row == first, 0.0, 1.0)
    mk[2] = jnp.where(col == nz - 1, 0.0, 1.0)
    mk[3] = jnp.where(col == 0, 0.0, 1.0)

    pl.semaphore_wait(barrier, n - 1)

    def p_view(e):
        return lambda planes, lines: xp.at[e, planes, lines]

    def u_view(e):
        return lambda planes, lines: xu.at[e, :, planes, lines]

    def q_view(e):
        return lambda planes, lines: qs.at[e, planes, lines]

    def wind_view(planes, lines):
        return raw.at[pl.ds(0, 3), planes, lines]

    def row_view(i):
        return lambda planes, lines: raw.at[i, planes, lines]

    every, across = (0, 1, 2, 3, 4), (0, 1, 3, 4)
    groups = [
        (p_view(0), WP, WP, every), (u_view(0), WU, WU, every),
        (row_view(3), WC, WC, every),
        (p_view(1), WP, WP, every), (u_view(1), WU, WU, every),
        (p_view(2), WP, WP, every), (u_view(2), WU, WU, every),
        (wind_view, WC, 1, every), (row_view(4), WC, 0, (2,)),
        (q_view(0), WQ, WQ, across), (q_view(1), WQ, WQ, across), (q_view(2), WQ, WQ, across),
    ]
    own_lines = pl.ds(0, cy)
    edge_lines = pl.ds(pl.multiple_of((1 - sub) * (cy - HALO), 8), HALO)
    halo_lines = pl.ds(cy, HALO)

    def remote(g, kind):
        view, base, w, _ = groups[g]
        end = base + cx
        if kind == 0:
            src, dst = view(pl.ds(end - w, w), own_lines), view(pl.ds(base - w, w), own_lines)
            target = {"slab": slab + 1}
        elif kind == 1:
            src, dst = view(pl.ds(base, w), own_lines), view(pl.ds(end, w), own_lines)
            target = {"slab": slab - 1}
        else:
            planes = (pl.ds(base, cx), pl.ds(base - w, w), pl.ds(end, w))[kind - 2]
            src, dst = view(planes, edge_lines), view(planes, halo_lines)
            target = {"sub": 1 - sub}
        return pltpu.make_async_remote_copy(
            src_ref=src, dst_ref=dst, send_sem=send.at[g, kind], recv_sem=recv.at[g, kind],
            device_id=target, device_id_type=MESH,
        )

    def begin(g, chosen=(0, 1, 2)):
        kinds = [kind for kind in groups[g][3] if kind in chosen]
        if 0 in kinds:
            pl.when(has_right)(lambda: remote(g, 0).start())
            pl.when(has_left)(lambda: remote(g, 1).start())
        if 2 in kinds:
            remote(g, 2).start()

    def forward(g):
        if 0 in groups[g][3]:
            pl.when(has_left)(lambda: remote(g, 0).wait_recv())
            remote(g, 3).start()
            pl.when(has_right)(lambda: remote(g, 1).wait_recv())
            remote(g, 4).start()

    def arrive(g, kinds=(2, 3, 4)):
        for kind in groups[g][3]:
            if kind in kinds:
                remote(g, kind).wait_recv()

    def finish(g):
        for kind in groups[g][3]:
            if kind == 0:
                pl.when(has_right)(lambda: remote(g, 0).wait_send())
            elif kind == 1:
                pl.when(has_left)(lambda: remote(g, 1).wait_send())
            else:
                remote(g, kind).wait_send()

    lane = lax.broadcasted_iota(jnp.int32, (1, LANES), 1)

    def reduce_start(e, parts):
        line = jnp.zeros((1, LANES), jnp.float32)
        for i, part in enumerate(parts):
            line = line + jnp.where(lane == i, jnp.sum(fold(part), keepdims=True), 0.0)
        red[e, me] = line

        def tell(at, core):
            pltpu.make_async_remote_copy(
                src_ref=red.at[e, me], dst_ref=red.at[e, me],
                send_sem=red_send.at[e], recv_sem=red_recv.at[e],
                device_id=(at, core), device_id_type=MESH,
            ).start()

        def push(k, carry):
            at = lax.rem(slab + k, slabs)
            for core in range(subs):
                tell(at, core)
            return carry

        lax.fori_loop(1, slabs, push, 0)
        for k in range(1, subs):
            tell(slab, lax.rem(sub + k, subs))

    def red_wait(e, sem):
        block = red.at[e, pl.ds(0, n - 1)]
        pltpu.make_async_copy(block, block, sem.at[e]).wait()

    def reduce_end(e, count):
        red_wait(e, red_recv)
        total = jnp.sum(red[e], axis=0)
        return [
            jnp.sum(jnp.where(lane == i, total, 0.0), axis=1, keepdims=True)
            for i in range(count)
        ]

    def turn(f):
        return (
            pltpu.roll(f, rows - 1, 0), pltpu.roll(f, 1, 0),
            pltpu.roll(f, nz - 1, 1), pltpu.roll(f, 1, 1),
        )

    def masked(f):
        yp, ym, zp, zm = turn(f)
        return yp * mk[0], ym * mk[1], zp * mk[2], zm * mk[3]

    def off_diagonal(below, around, above, k):
        yp, ym, zp, zm = around
        total = co[0, k] * above + co[1, k] * below
        total = total + (co[2, k] * yp + co[3, k] * ym)
        return total + (co[4, k] * zp + co[5, k] * zm)

    def loop(count, body, init=0, low=0):
        step = max(u for u in range(1, UNROLL + 1) if count % u == 0)

        def several(k, carry):
            for i in range(step):
                carry = body(low + k * step + i, carry)
            return carry

        return lax.fori_loop(0, count // step, several, init)

    def spans(spans_of, body):
        for low, high in spans_of:
            if high > low:
                loop(high - low, body, low=low)

    def inside(k, w):
        at = slab * cx + k - w
        return jnp.logical_and(at >= 0, at < slabs * cx)

    def coefficients(where):
        def body(k, carry):
            ok = jnp.where(inside(k, WC), 1.0, 0.0)
            keep = jnp.full((rows, nz), ok) > 0.5
            hx, hy, hz = 0.5 * raw[0, k], 0.5 * raw[1, k], 0.5 * raw[2, k]
            co[0, k] = 1.0 - hx
            co[1, k] = 1.0 + hx
            co[2, k] = (1.0 - hy) * mk[0]
            co[3, k] = (1.0 + hy) * mk[1]
            co[4, k] = (1.0 - hz) * mk[2]
            co[5, k] = (1.0 + hz) * mk[3]
            diagonal = 6.0 + raw[3, k]
            co[6, k] = diagonal
            co[7, k] = jnp.where(keep, 1.0 / diagonal, 0.0)
            co[8, k] = jnp.where(keep, 1.0 / raw[4, k], 0.0)
            return carry

        spans(where, body)

    def first_guess(p):
        def body(k, carry):
            here = p[k + 1]
            yp, ym, zp, zm = masked(here)
            total = (p[k] + p[k + 2]) + (yp + ym) + (zp + zm)
            ok = jnp.where(inside(k, WP - 1), 1.0 / 7.0, 0.0)
            t1[k] = (here + total * (1.0 / 7.0)) * ok
            return carry

        loop(cx + 2 * (WP - 1), body)

    def schur(qq):
        def body(k, carry):
            here = t1[k + 1]
            off = off_diagonal(t1[k], turn(here), t1[k + 2], k + WC)
            qq[k + WQ] = (off - co[6, k + WC] * here) * co[8, k + WC]
            return carry

        loop(cx, body)

    def velocity_first(qq, u, where):
        def body(k, carry):
            yp, ym, zp, zm = masked(qq[k + 1])
            scale = co[7, k]
            y0[0, k] = (u[0, k] - 0.5 * (qq[k + 2] - qq[k])) * scale
            y0[1, k] = (u[1, k] - 0.5 * (yp - ym)) * scale
            y0[2, k] = (u[2, k] - 0.5 * (zp - zm)) * scale
            return carry

        spans(where, body)

    def velocity_second(where):
        def body(k, carry):
            scale = co[7, k + 1]
            for c in range(3):
                here = y0[c, k + 1]
                off = off_diagonal(y0[c, k], turn(here), y0[c, k + 2], k + 1)
                y1[c, k] = here + off * scale
            return carry

        spans(where, body)

    def image(e, qq, vectors):
        def body(k, acc):
            q = qq[k + WQ]
            qa, qb = qq[k + WQ + 1], qq[k + WQ - 1]
            yp, ym, zp, zm = masked(q)
            grads = (0.5 * (qa - qb), 0.5 * (yp - ym), 0.5 * (zp - zm))
            low = 0.5 * ((qa + qb) + (yp + ym) + (zp + zm)) - 3.0 * q
            out = []
            for c in range(3):
                here = y1[c, k + 1]
                below, above = y1[c, k], y1[c, k + 2]
                around = turn(here)
                off = off_diagonal(below, around, above, k + WC)
                w = (co[6, k + WC] * here - off + grads[c])[:cy]
                if c == 0:
                    low = low - 0.5 * (above - below)
                elif c == 1:
                    low = low - 0.5 * (around[0] * mk[0] - around[1] * mk[1])
                else:
                    low = low - 0.5 * (around[2] * mk[2] - around[3] * mk[3])
                os_[e, c, k] = here[:cy]
                out.append(w)
            os_[e, 3, k] = q[:cy]
            out.append(low[:cy])
            if e + 1 < ITERS:
                for c in range(3):
                    xu[e + 1, c, k + WU, 0:cy] = out[c]
                xp[e + 1, k + WP, 0:cy] = out[3]
            else:
                for c in range(4):
                    wl[c, k] = out[c]
            acc = list(acc)
            for i, (p, u) in enumerate(vectors):
                held = [u[c, k + WU, 0:cy] for c in range(3)] + [p[k + WP, 0:cy]]
                term = held[0] * out[0] + held[1] * out[1]
                acc[i + 1] = acc[i + 1] + (term + (held[2] * out[2] + held[3] * out[3]))
                if i == e:
                    term = held[0] * held[0] + held[1] * held[1]
                    acc[0] = acc[0] + (term + (held[2] * held[2] + held[3] * held[3]))
            return tuple(acc)

        zero = jnp.zeros((cy, nz), jnp.float32)
        acc = (zero,) * (e + 2)
        acc = loop(WP, body, acc)
        acc = loop(WP, body, acc, low=cx - WP)
        if e + 1 < ITERS:
            begin((3, 5)[e], (0, 1))
        acc = loop(cx - 2 * WP, body, acc, low=WP)
        if e + 1 < ITERS:
            begin((3, 5)[e], (2,))
        return acc

    def write_out(e):
        return (
            pltpu.make_async_copy(ob.at[e], basis.at[e], store.at[0, e]),
            pltpu.make_async_copy(os_.at[e], search.at[e], store.at[1, e]),
        )

    def results(e, vector, inverse):
        p, u = vector

        def body(k, carry):
            for c in range(3):
                ob[e, c, k] = u[c, k + WU, 0:cy] * inverse
            ob[e, 3, k] = p[k + WP, 0:cy] * inverse
            for c in range(4):
                os_[e, c, k] = os_[e, c, k] * inverse
            return carry

        loop(cx, body)
        for item in write_out(e):
            item.start()

    loads[0].wait()
    begin(0)
    for item in loads[2:]:
        item.wait()
    for g in (2, 7, 8):
        begin(g, (2,))
    loads[1].wait()
    begin(1)
    for g in (2, 7):
        begin(g, (0, 1))
    for g in (2, 7, 8):
        arrive(g, (2,))
    coefficients([(WC, WC + cx)])
    forward(0)
    arrive(0)

    vectors = [(xp.at[0], xu.at[0])]
    inverses = []
    entries = {}
    first_guess(vectors[0][0])
    for e in range(ITERS):
        p, u = vectors[e]
        p_group, u_group = ((0, 1), (3, 4), (5, 6))[e]
        if e > 0:
            first_guess(p)
        qq = qs.at[e]
        schur(qq)
        begin(9 + e)
        if e > 0:
            results(e - 1, vectors[e - 1], inverses[e - 1])
        end_u, end_1 = cx + 2 * WU, cx + 2
        deep = min(3, end_1 // 2)
        inner = (WU + 1, WU + cx - 1)
        arrive(u_group, (2,))
        if e > 0:

            def form_u(k, carry, e=e):
                for c in range(3):
                    total = xu[e, c, k] * factor
                    for g, (_, other) in zip(weights, vectors[:e]):
                        total = total - g * other[c, k]
                    u[c, k] = total
                return carry

            spans([(WU, WU + cx)], form_u)
        velocity_first(qq, u, [inner])
        velocity_second([(deep, end_1 - deep)])
        forward(u_group)
        if e == 0:
            for g in (2, 7):
                forward(g)
            for g in (2, 7):
                arrive(g, (3, 4))
            coefficients([(0, WC), (WC + cx, cx + 2 * WC)])
        forward(9 + e)
        arrive(u_group, (3, 4))
        if e > 0:
            spans([(0, WU), (WU + cx, end_u)], form_u)
        arrive(9 + e)
        velocity_first(qq, u, [(0, inner[0]), (inner[1], end_u)])
        velocity_second([(0, deep), (end_1 - deep, end_1)])
        acc = image(e, qq, vectors)
        reduce_start(e, acc)
        if e + 1 < ITERS:
            begin(u_group + 3 if e == 0 else 6)
        sums = reduce_end(e, e + 2)
        norm = jnp.sqrt(sums[0])
        factor = 1.0 / norm
        if e > 0:
            entries[(e, e - 1)] = norm
        inverses.append(factor)
        weights = []
        for i in range(e + 1):
            h = sums[i + 1] * inverses[i] * factor
            entries[(i, e)] = h
            weights.append(h * inverses[i])
        if e + 1 < ITERS:
            g_p = (3, 5)[e]
            forward(g_p)
            arrive(g_p)
            new = (vp.at[e], vu.at[e])

            def form_p(k, carry, e=e):
                total = xp[e + 1, k] * factor
                for g, (other, _) in zip(weights, vectors[: e + 1]):
                    total = total - g * other[k]
                vp[e, k] = total
                return carry

            loop(cx + 2 * WP, form_p)
            vectors.append(new)

    def close(k, acc):
        for c in range(4):
            total = wl[c, k] * factor
            for g, (p, u) in zip(weights, vectors):
                held = p[k + WP, 0:cy] if c == 3 else u[c, k + WU, 0:cy]
                total = total - g * held
            ob[ITERS, c, k] = total
            acc = acc + total * total
        return acc

    acc = loop(cx, close, jnp.zeros((cy, nz), jnp.float32))
    reduce_start(ITERS, [acc])
    results(ITERS - 1, vectors[ITERS - 1], inverses[ITERS - 1])
    for g in range(len(groups)):
        finish(g)
    norm = jnp.sqrt(reduce_end(ITERS, 1)[0])
    entries[(ITERS, ITERS - 1)] = norm
    factor = 1.0 / norm

    def scale(k, carry):
        for c in range(4):
            ob[ITERS, c, k] = ob[ITERS, c, k] * factor
        return carry

    loop(cx, scale)
    final = pltpu.make_async_copy(ob.at[ITERS], basis.at[ITERS], store.at[0, ITERS])
    final.start()
    r = lax.broadcasted_iota(jnp.int32, (ITERS + 1, ITERS), 0)
    c = lax.broadcasted_iota(jnp.int32, (ITERS + 1, ITERS), 1)
    table = jnp.zeros((ITERS + 1, ITERS), jnp.float32)
    for (i, j), value in entries.items():
        table = table + jnp.where(jnp.logical_and(r == i, c == j), value, 0.0)
    hess[...] = table
    for e in range(ITERS + 1):
        red_wait(e, red_send)
    for e in range(ITERS):
        for item in write_out(e):
            item.wait()
    final.wait()


def per_device(slabs, subs, start, wind, reaction, mass):
    _, cx, cy, nz = start.shape
    n = slabs * subs
    rows = cy + HALO
    f32 = jnp.float32

    def field(*lead):
        return pltpu.VMEM((*lead, rows, nz), f32)

    out_shape = (
        jax.ShapeDtypeStruct((ITERS + 1, 4, cx, cy, nz), f32),
        jax.ShapeDtypeStruct((ITERS, 4, cx, cy, nz), f32),
        jax.ShapeDtypeStruct((ITERS + 1, ITERS), f32),
    )
    anywhere = pl.BlockSpec(memory_space=pl.ANY)
    return pl.pallas_call(
        functools.partial(kernel, slabs, subs, cx, cy, nz),
        out_shape=out_shape,
        in_specs=[pl.BlockSpec(memory_space=pltpu.HBM)] * 4,
        out_specs=(anywhere, anywhere, pl.BlockSpec(memory_space=pltpu.VMEM)),
        scratch_shapes=[
            field(ITERS, cx + 2 * WP),
            field(ITERS, 3, cx + 2 * WU),
            field(ITERS - 1, cx + 2 * WP),
            field(ITERS - 1, 3, cx + 2 * WU),
            field(5, cx + 2 * WC),
            field(9, cx + 2 * WC),
            field(4),
            field(cx + 2 * (WP - 1)),
            field(ITERS, cx + 2 * WQ),
            field(3, cx + 2 * WU),
            field(3, cx + 2),
            pltpu.VMEM((4, cx, cy, nz), f32),
            pltpu.VMEM((ITERS + 1, 4, cx, cy, nz), f32),
            pltpu.VMEM((ITERS, 4, cx, cy, nz), f32),
            pltpu.VMEM((ITERS + 1, n, 1, LANES), f32),
            pltpu.SemaphoreType.DMA((12, 5)),
            pltpu.SemaphoreType.DMA((12, 5)),
            pltpu.SemaphoreType.DMA((ITERS + 1,)),
            pltpu.SemaphoreType.DMA((ITERS + 1,)),
            pltpu.SemaphoreType.DMA((5,)),
            pltpu.SemaphoreType.DMA((2, ITERS + 1)),
        ],
        compiler_params=pltpu.CompilerParams(
            collective_id=0, has_side_effects=True, vmem_limit_bytes=63_900_000
        ),
    )(start, wind, reaction, mass)


def solution(mesh):
    slabs, subs = mesh.shape["slab"], mesh.shape["sub"]
    return jax.shard_map(
        functools.partial(per_device, slabs, subs),
        mesh=mesh,
        in_specs=(
            P(None, "slab", "sub", None),
            P(None, "slab", "sub", None),
            P("slab", "sub", None),
            P("slab", "sub", None),
        ),
        out_specs=(P(None, None, "slab", "sub", None), P(None, None, "slab", "sub", None), P()),
        check_vma=False,
    )
```
